32 devices in a mesh: modes: 8 (over z, y), cheb: 4 (over x, core).
Axes of the slice: x: 2, y: 2, z: 4, core: 2. Of those that a mesh axis runs over, the one named last changes fastest.
Arguments:
- start: float32 [2, 2, 2048, 256], P(None, None, ('modes', 'cheb')), may hold values from -45 to 45
- forcing: float32 [2, 2, 2048, 256], P(None, None, ('modes', 'cheb')), may hold values from -45 to 45
- taus: float32 [2048, 256, 256], P(('modes', 'cheb')), may hold values from -5 to 5
Outputs:
- solution: float32 [2, 2, 2048, 256], P(None, None, ('modes', 'cheb'))
The draws below stay inside these ranges and needn't reach their ends.
All inputs are finite; a program needn't handle non-finite values.
Results may differ from the reference program's by a relative error of at most 0.0002.
Values sent between devices are 32-bit elements; how exact they have to be, the bound alone decides.
A program may use at most 128 MiB of HBM per device.

```python
import math
import jax
import jax.numpy as jnp
from jax import lax

KX = 2048
NY = 256
BATCH = 2
NEWTON = 2
KRYLOV = 3


def spectral_field(key):
    subkeys = jax.random.split(key, 3)
    entries = jnp.clip(jax.random.normal(subkeys[0], (BATCH, 2, KX, NY), jnp.float32), -5.0, 5.0)
    log_low = math.log(0.3)
    log_high = math.log(3.0)
    mode_scale = jnp.exp(jax.random.uniform(subkeys[1], (1, 1, KX, 1), jnp.float32, log_low, log_high))
    degree_scale = jnp.exp(jax.random.uniform(subkeys[2], (1, 1, 1, NY), jnp.float32, log_low, log_high))
    return entries * mode_scale * degree_scale


def draw_start(key, part):
    return spectral_field(jax.random.fold_in(key, 11))


def draw_forcing(key, part):
    return spectral_field(jax.random.fold_in(key, 23))


def draw_taus(key, part):
    subkeys = jax.random.split(jax.random.fold_in(key, 37), 3)
    wavenumber = 16.0 * jnp.arange(KX, dtype=jnp.int32).astype(jnp.float32) / KX
    envelope = 1.0 / (1.0 + wavenumber * wavenumber / 16.0)
    rough = jnp.exp(jax.random.uniform(subkeys[0], (KX,), jnp.float32, math.log(0.5), math.log(2.0)))
    diagonal = jnp.exp(jax.random.uniform(subkeys[1], (KX, NY), jnp.float32, math.log(0.5), math.log(2.0)))
    offdiag = jnp.clip(jax.random.normal(subkeys[2], (KX, NY, NY), jnp.float32), -5.0, 5.0)
    matrix = offdiag * (0.3 / math.sqrt(NY)) + diagonal[:, :, None] * jnp.eye(NY, dtype=jnp.float32)[None, :, :]
    return matrix * (envelope * rough)[:, None, None]


def setup_inputs(seed: int = 0) -> dict:
    streams_of = jax.random.split(jax.random.key(seed), 4)
    return {
        "start": draw_start(jax.random.fold_in(streams_of[3], 71), 0),
        "forcing": draw_forcing(jax.random.fold_in(streams_of[3], 71), 0),
        "taus": draw_taus(jax.random.fold_in(streams_of[3], 71), 0),
    }


HIGH = lax.Precision.HIGHEST
STRENGTH = 0.1

def cheb_rows(degree_count):
    degree = jnp.arange(degree_count, dtype=jnp.int32)[:, None]
    node = 2 * jnp.arange(degree_count, dtype=jnp.int32)[None, :] + 1
    turns = degree * node % (4 * degree_count)
    return jnp.cos(2.0 * math.pi / (4 * degree_count) * turns.astype(jnp.float32))

def sample_grid(values):
    spectrum = lax.complex(values[:, 0], values[:, 1])
    spectrum = jnp.concatenate([spectrum, jnp.zeros_like(spectrum[:, :1])], axis=1)
    return jnp.fft.irfft(spectrum, n=2 * KX, axis=1) * (2 * KX / math.sqrt(KX * NY))

def to_points(coefs, cheb_table):
    values = jnp.einsum('brkn,ni->brki', coefs, cheb_table, precision=HIGH)
    wavenumber = (16.0 * jnp.arange(KX, dtype=jnp.int32).astype(jnp.float32) / KX)[:, None]
    slopes = jnp.stack([-wavenumber * values[:, 1], wavenumber * values[:, 0]], axis=1)
    return (sample_grid(values), sample_grid(slopes))

def to_coefficients(points, cheb_table):
    spectrum = jnp.fft.rfft(points, axis=1)[:, :KX] / (2 * KX)
    parts = jnp.stack([jnp.real(spectrum), jnp.imag(spectrum)], axis=1).astype(points.dtype)
    weights = (jnp.where(jnp.arange(NY) == 0, 1.0, 2.0) / NY).astype(points.dtype)
    coefs = jnp.einsum('brki,ni->brkn', parts, cheb_table, precision=HIGH)
    return coefs * weights * math.sqrt(KX * NY)

def precondition(coefs, taus):
    tau_keep = (jnp.arange(NY) < NY - 2).astype(coefs.dtype)
    return jnp.einsum('kam,brkm->brka', taus, coefs * tau_keep, precision=HIGH)

def least_squares(hessen, beta_norm):
    steps_count = len(hessen)
    matrix = [[hessen[col_index][:, row_index] for row_index in range(col_index + 2)] for col_index in range(steps_count)]
    target = [beta_norm] + [jnp.zeros_like(beta_norm) for row_index in range(steps_count)]
    cosines = []
    sines_list = []
    for col_index in range(steps_count):
        column = matrix[col_index]
        for row_index in range(col_index):
            upper_entry = cosines[row_index] * column[row_index] + sines_list[row_index] * column[row_index + 1]
            lower_entry = cosines[row_index] * column[row_index + 1] - sines_list[row_index] * column[row_index]
            column[row_index] = upper_entry
            column[row_index + 1] = lower_entry
        radius = jnp.sqrt(column[col_index] * column[col_index] + column[col_index + 1] * column[col_index + 1])
        cosines.append(column[col_index] / radius)
        sines_list.append(column[col_index + 1] / radius)
        column[col_index] = radius
        target[col_index + 1] = -sines_list[col_index] * target[col_index]
        target[col_index] = cosines[col_index] * target[col_index]
    solved = [None] * steps_count
    for row_index in reversed(range(steps_count)):
        partial_sum = target[row_index]
        for col_index in range(row_index + 1, steps_count):
            partial_sum = partial_sum - matrix[col_index][row_index] * solved[col_index]
        solved[row_index] = partial_sum / matrix[row_index][row_index]
    return solved

def reference(start, forcing, taus):
    cheb_table = cheb_rows(NY)
    iterate = start
    for newton_step in range(NEWTON):
        base_points, base_slopes = to_points(iterate, cheb_table)
        residual = iterate + precondition(to_coefficients(STRENGTH * base_points * base_slopes, cheb_table) - forcing, taus)
        beta_norm = jnp.sqrt(lax.optimization_barrier(jnp.sum(residual * residual, axis=(1, 2, 3))))
        krylov_basis = [-residual / beta_norm[:, None, None, None]]
        hessen = []
        for column in range(KRYLOV):
            probe_points, probe_slopes = to_points(krylov_basis[column], cheb_table)
            product = STRENGTH * (base_points * probe_slopes + probe_points * base_slopes)
            applied = krylov_basis[column] + precondition(to_coefficients(product, cheb_table), taus)
            projections = jnp.stack([lax.optimization_barrier(jnp.sum(vector * applied, axis=(1, 2, 3))) for vector in krylov_basis], axis=1)
            for index, vector in enumerate(krylov_basis):
                applied = applied - projections[:, index][:, None, None, None] * vector
            length = jnp.sqrt(lax.optimization_barrier(jnp.sum(applied * applied, axis=(1, 2, 3))))
            hessen.append(jnp.concatenate([projections, length[:, None]], axis=1))
            krylov_basis.append(applied / length[:, None, None, None])
        solved = least_squares(hessen, beta_norm)
        for column in range(KRYLOV):
            iterate = iterate + solved[column][:, None, None, None] * krylov_basis[column]
    return iterate
```

```python
import functools
import math

import jax
import jax.numpy as jnp
import numpy as np
from jax import lax
from jax.experimental import pallas as pl
from jax.experimental.pallas import tpu as pltpu
from jax.sharding import PartitionSpec as P

NEWTON = 2
KRYLOV = 3


PREC = lax.Precision.HIGH
STRENGTH = 0.1
AXES = ("modes", "cheb")
STAT_LANES = 128
LANES = 128


def cheb_rows(degree_count):
    degree = jnp.arange(degree_count, dtype=jnp.int32)[:, None]
    node = 2 * jnp.arange(degree_count, dtype=jnp.int32)[None, :] + 1
    turns = degree * node % (4 * degree_count)
    return jnp.cos(2.0 * math.pi / (4 * degree_count) * turns.astype(jnp.float32))


def phase_table(row_count, col_count, period):
    row_index = jnp.arange(row_count, dtype=jnp.int32)[:, None]
    col_index = jnp.arange(col_count, dtype=jnp.int32)[None, :]
    turns = row_index * col_index % period
    angle = 2.0 * math.pi / period * turns.astype(jnp.float32)
    return (jnp.cos(angle), jnp.sin(angle))


def least_squares(hessen, beta_norm):
    steps_count = len(hessen)
    matrix = [
        [hessen[col_index][:, row_index] for row_index in range(col_index + 2)]
        for col_index in range(steps_count)
    ]
    target = [beta_norm] + [jnp.zeros_like(beta_norm) for row_index in range(steps_count)]
    cosines = []
    sines_list = []
    for col_index in range(steps_count):
        column = matrix[col_index]
        for row_index in range(col_index):
            upper_entry = (
                cosines[row_index] * column[row_index]
                + sines_list[row_index] * column[row_index + 1]
            )
            lower_entry = (
                cosines[row_index] * column[row_index + 1]
                - sines_list[row_index] * column[row_index]
            )
            column[row_index] = upper_entry
            column[row_index + 1] = lower_entry
        radius = jnp.sqrt(
            column[col_index] * column[col_index] + column[col_index + 1] * column[col_index + 1]
        )
        cosines.append(column[col_index] / radius)
        sines_list.append(column[col_index + 1] / radius)
        column[col_index] = radius
        target[col_index + 1] = -sines_list[col_index] * target[col_index]
        target[col_index] = cosines[col_index] * target[col_index]
    solved = [None] * steps_count
    for row_index in reversed(range(steps_count)):
        partial_sum = target[row_index]
        for col_index in range(row_index + 1, steps_count):
            partial_sum = partial_sum - matrix[col_index][row_index] * solved[col_index]
        solved[row_index] = partial_sum / matrix[row_index][row_index]
    return solved


def shards(start, forcing, taus):
    group_size = lax.axis_size(AXES)
    batch, parts, local_modes, degrees = start.shape
    total_modes = local_modes * group_size
    points_count = 2 * total_modes
    outer_len = max(2 ** ((points_count.bit_length() - 1) // 2), local_modes)
    inner_len = points_count // outer_len
    half_inner = inner_len // 2
    split = outer_len // local_modes
    rows = degrees // group_size
    block_lanes = batch * 2 * local_modes
    fields = rows * batch
    spread = 1.0 / math.sqrt(total_modes * degrees)
    gather_factor = math.sqrt(total_modes * degrees) / points_count
    cheb_table = cheb_rows(degrees)
    tau_keep = (jnp.arange(degrees) < degrees - 2).astype(jnp.float32)
    coef_weights = jnp.where(jnp.arange(degrees) == 0, 1.0, 2.0).astype(jnp.float32) / degrees
    back_table = cheb_table * (coef_weights * tau_keep)[:, None]

    section_cos, section_sin = phase_table(inner_len, half_inner, inner_len)
    value_table = jnp.stack([section_cos, section_sin])
    slope_table = jnp.stack([-section_sin, section_cos])
    back_cos, back_sin = section_cos.T, section_sin.T
    twist_cos, twist_sin = phase_table(inner_len, outer_len, points_count)
    final_cos, final_sin = phase_table(outer_len, outer_len, outer_len)
    turn_cos = (
        twist_cos[:, :, None] * final_cos[None] - twist_sin[:, :, None] * final_sin[None]
    )
    turn_sin = (
        twist_sin[:, :, None] * final_cos[None] + twist_cos[:, :, None] * final_sin[None]
    )
    turn_table = lax.optimization_barrier(
        jnp.concatenate([turn_cos, -turn_sin, -turn_sin, -turn_cos], axis=1)
    )
    mode = (
        outer_len * jnp.arange(half_inner, dtype=jnp.int32)[:, None]
        + jnp.arange(outer_len, dtype=jnp.int32)[None, :]
    )
    paired_mode = jnp.concatenate([mode, mode], axis=1)[:, None, :]
    weights = jnp.where(paired_mode == 0, 1.0, 2.0).astype(jnp.float32) * spread
    slope_weights = weights * (16.0 * paired_mode.astype(jnp.float32) / total_modes)

    def exchange(blocks):
        return lax.all_to_all(blocks, AXES, split_axis=0, concat_axis=0, tiled=True)

    def stat_block(stats):
        flat = jnp.pad(stats.reshape(-1), (0, STAT_LANES - stats.size))
        return jnp.broadcast_to(flat, (group_size, rows, STAT_LANES))

    def read_stats(received, shape):
        flat = jnp.sum(received[:, 0, :], axis=0)
        return flat[: math.prod(shape)].reshape(shape)

    def to_points(coefs, stats):
        values = jnp.einsum("ni,brkn->ibrk", cheb_table, coefs, precision=PREC)
        blocks = values.reshape(group_size, rows, block_lanes)
        if stats is not None:
            blocks = jnp.concatenate([blocks, stat_block(stats)], axis=2)
        received = exchange(blocks)
        summed = None
        if stats is not None:
            summed = read_stats(received[:, :, block_lanes:], stats.shape)
            received = received[:, :, :block_lanes]
        spectrum = received.reshape(half_inner, split, rows, batch, 2, local_modes)
        spectrum = spectrum.transpose(0, 2, 3, 4, 1, 5).reshape(
            half_inner, fields, 2 * outer_len
        )

        def points_of(table, weighted):
            turned = jnp.einsum("sjq,qyl->jysl", table, weighted, precision=PREC)
            turned = turned.reshape(inner_len, fields, 4 * outer_len)
            return jnp.einsum("jyl,jlt->jyt", turned, turn_table, precision=PREC)

        values = points_of(value_table, spectrum * weights)
        slopes = points_of(slope_table, spectrum * slope_weights)
        return (values, slopes), summed

    def to_coefficients(points):
        turned = jnp.einsum("jyt,jlt->jyl", points, turn_table, precision=PREC) * gather_factor
        direct = turned[:, :, : 2 * outer_len].reshape(inner_len, -1)
        swapped = turned[:, :, 2 * outer_len :].reshape(inner_len, -1)
        spectrum = jnp.dot(back_cos, direct, precision=PREC) + jnp.dot(
            back_sin, swapped, precision=PREC
        )
        blocks = spectrum.reshape(half_inner, rows, batch, 2, split, local_modes)
        blocks = blocks.transpose(0, 4, 1, 2, 3, 5).reshape(group_size, rows, block_lanes)
        received = exchange(blocks).reshape(degrees, batch, 2, local_modes)
        return jnp.einsum("ibrk,ni->brkn", received, back_table, precision=PREC)

    def precondition(coefs):
        return jnp.einsum("kam,brkm->brka", taus, coefs, precision=PREC)

    def on_points(scale):
        return jnp.tile(scale, rows)[None, :, None]

    def on_coefs(scale):
        return scale[:, None, None, None]

    iterate = start
    kept_forcing = forcing * tau_keep
    base, nothing = to_points(iterate, None)
    for newton_step in range(NEWTON):
        base_points, base_slopes = base
        residual = iterate + precondition(
            to_coefficients(STRENGTH * base_points * base_slopes) - kept_forcing
        )
        local_square = jnp.sum(residual * residual, axis=(1, 2, 3))
        image, squared = to_points(residual, local_square)
        beta_norm = jnp.sqrt(squared)
        krylov_basis = [-residual / on_coefs(beta_norm)]
        images = [tuple(-part / on_points(beta_norm) for part in image)]
        hessen = []
        for column in range(KRYLOV):
            probe_points, probe_slopes = images[column]
            product = STRENGTH * (base_points * probe_slopes + probe_points * base_slopes)
            applied = krylov_basis[column] + precondition(to_coefficients(product))
            local_stats = jnp.stack(
                [jnp.sum(vector * applied, axis=(1, 2, 3)) for vector in krylov_basis + [applied]],
                axis=1,
            )
            last = column == KRYLOV - 1
            if last:
                stats = read_stats(exchange(stat_block(local_stats)), local_stats.shape)
            else:
                image, stats = to_points(applied, local_stats)
            projections, square = stats[:, :-1], stats[:, -1]
            length = jnp.sqrt(square - jnp.sum(projections * projections, axis=1))
            hessen.append(jnp.concatenate([projections, length[:, None]], axis=1))
            if not last:
                for index in range(column + 1):
                    applied = applied - on_coefs(projections[:, index]) * krylov_basis[index]
                    image = tuple(
                        part - on_points(projections[:, index]) * known
                        for part, known in zip(image, images[index])
                    )
                krylov_basis.append(applied / on_coefs(length))
                images.append(tuple(part / on_points(length) for part in image))
        solved = least_squares(hessen, beta_norm)
        for column in range(KRYLOV):
            iterate = iterate + on_coefs(solved[column]) * krylov_basis[column]
            base = tuple(
                part + on_points(solved[column]) * known
                for part, known in zip(base, images[column])
            )
    return iterate


def split_table(table):
    table = np.asarray(table, np.float32)
    high = table.astype(jnp.bfloat16)
    low = (table - high.astype(np.float32)).astype(jnp.bfloat16)
    return high, low


def left_table(table):
    high, low = split_table(table)
    return np.concatenate([high, low, high], axis=1)


def tables_of(local_modes, group_size, degrees):
    total = local_modes * group_size
    points = 2 * total
    inner = points // local_modes
    half = local_modes // 2
    spread = 1.0 / math.sqrt(total * degrees)
    degree = np.arange(degrees)[:, None]
    node = 2 * np.arange(degrees)[None, :] + 1
    cheb = np.cos(2.0 * np.pi / (4 * degrees) * (degree * node % (4 * degrees)))
    coef_weights = np.where(np.arange(degrees) == 0, 1.0, 2.0) / degrees
    keep = np.arange(degrees) < degrees - 2
    to_rows = left_table(cheb.T)
    to_degrees = left_table(cheb * (coef_weights * keep)[:, None])

    j_low = np.arange(inner)[:, None]
    source = np.arange(group_size)[None, :]
    angle = 2.0 * np.pi / inner * (j_low * source % inner)
    cos, sin = np.cos(angle), np.sin(angle)
    real = np.concatenate([cos, -sin], axis=1)
    imag = np.concatenate([sin, cos], axis=1)
    wave = np.tile(16.0 * local_modes * source / total, (1, 2))
    gather = 2.0 * spread * np.concatenate([real, imag, real * wave, imag * wave], axis=0)
    gather = left_table(gather)
    scatter = np.concatenate(
        [np.concatenate([cos.T, sin.T], axis=1), np.concatenate([-sin.T, cos.T], axis=1)], axis=0
    )
    scatter = left_table(scatter * math.sqrt(total * degrees) / points)

    lane_mode = np.tile(np.arange(local_modes), 2)[None, :]
    twist = 2.0 * np.pi / points * (j_low * lane_mode)
    wave_low = np.broadcast_to(16.0 * lane_mode / total, twist.shape)
    twist = np.stack([np.cos(twist), np.sin(twist), wave_low]).astype(np.float32)

    mode = np.arange(local_modes)
    final = 2.0 * np.pi / local_modes * (mode[:, None] * mode[None, :] % local_modes)
    pair = np.eye(2)
    cos_high, cos_low = split_table(np.kron(pair, np.cos(final)))
    sin_high, sin_low = split_table(np.kron(pair, np.sin(final)))
    cos_row = np.concatenate([cos_high, cos_low], axis=1)
    sin_row = np.concatenate([-sin_high, -sin_low], axis=1)
    finish = np.concatenate([cos_row, sin_row, cos_row, sin_row], axis=0)
    high_row = np.concatenate([cos_high, -sin_high], axis=1)
    low_row = np.concatenate([cos_low, -sin_low], axis=1)
    begin = np.concatenate([high_row, high_row, low_row], axis=0)
    return to_rows, to_degrees, gather, scatter, twist, finish, begin


def split(value):
    high = value.astype(jnp.bfloat16)
    return high, (value - high.astype(jnp.float32)).astype(jnp.bfloat16)


def right_operand(value):
    high, low = split(value)
    return jnp.concatenate([high, high, low], axis=0)


def dot(left, right):
    return jnp.dot(left, right, preferred_element_type=jnp.float32)


def flow_solver(
    sizes,
    start_ref,
    forcing_ref,
    taus_ref,
    to_rows_ref,
    to_degrees_ref,
    gather_ref,
    scatter_ref,
    twist_ref,
    finish_ref,
    begin_ref,
    out_ref,
    tau_terms,
    stage,
    vectors,
    applied,
    right,
    images,
    image,
    out_fwd,
    in_fwd,
    out_back,
    in_back,
    out_stat,
    in_stat,
    history,
    stage_sem,
    fwd_send,
    fwd_recv,
    back_send,
    back_recv,
    stat_send,
    stat_recv,
):
    group_size, minor, local_modes, rows, degrees, inner = sizes
    half = local_modes // 2
    me = lax.axis_index(AXES[0]) * minor + lax.axis_index(AXES[1])
    lane = lax.broadcasted_iota(jnp.int32, (1, LANES), 1)
    first_half = lane % local_modes < half
    low_flow = lane < local_modes

    def own_rows(index):
        return pl.ds(pl.multiple_of(index * rows, rows), rows)

    def exchange(src, dst, send_sem, recv_sem):
        def step(offset, carry):
            peer = lax.rem(me + offset, group_size)
            pltpu.make_async_remote_copy(
                src_ref=src.at[:, own_rows(peer), :],
                dst_ref=dst.at[:, own_rows(me), :],
                send_sem=send_sem,
                recv_sem=recv_sem,
                device_id=(peer // minor, lax.rem(peer, minor)),
                device_id_type=pl.DeviceIdType.MESH,
            ).start()
            return carry

        pltpu.make_async_copy(
            src.at[:, own_rows(me), :], dst.at[:, own_rows(me), :], recv_sem
        ).start()
        lax.fori_loop(1, group_size, step, 0)

    def finish_exchange(src, dst, send_sem, recv_sem):
        sent = pl.ds(0, (group_size - 1) * rows)
        pltpu.make_async_copy(src.at[:, sent, :], dst.at[:, sent, :], send_sem).wait()
        pltpu.make_async_copy(src, dst, recv_sem).wait()

    def to_modes(first, second):
        turned = pltpu.roll(second, half, 1)
        back = pltpu.roll(first, LANES - half, 1)
        return jnp.where(first_half, first, turned), jnp.where(first_half, back, second)

    def send_values(first, second):
        operand = right_operand(jnp.concatenate([first, second], axis=1))
        values = dot(to_rows_ref[...], operand)
        wide = lax.broadcasted_iota(jnp.int32, (1, 2 * LANES), 1)
        constant = jnp.logical_and(me == 0, wide % half == 0)
        constant = jnp.logical_and(constant, wide < LANES)
        values = values * jnp.where(constant, 0.5, 1.0)
        out_fwd[0] = values[:, :LANES]
        out_fwd[1] = values[:, LANES:]
        exchange(out_fwd, in_fwd, fwd_send, fwd_recv)

    def points_of_rows(pair):
        columns = []
        for row in (2 * pair, 2 * pair + 1):
            picked = pl.ds(row, group_size, stride=rows)
            real, imag = to_modes(in_fwd[0, picked, :], in_fwd[1, picked, :])
            columns.append(jnp.concatenate([real, imag], axis=0))
        operand = right_operand(jnp.concatenate(columns, axis=1))
        summed = dot(gather_ref[...], operand)
        cos, sin, low = twist_ref[0], twist_ref[1], twist_ref[2]
        lefts = []
        for index in range(2):
            part = summed[:, index * LANES : (index + 1) * LANES]
            real, imag, wave_real, wave_imag = (
                part[n * inner : (n + 1) * inner] for n in range(4)
            )
            slope_real = -(wave_imag + low * imag)
            slope_imag = wave_real + low * real
            for re, im in ((real, imag), (slope_real, slope_imag)):
                re_high, re_low = split(re * cos - im * sin)
                im_high, im_low = split(re * sin + im * cos)
                lefts.append(jnp.concatenate([re_high, im_high, re_low, im_low], axis=1))
        wide = dot(jnp.concatenate(lefts, axis=0), finish_ref[...])
        points = wide[:, :LANES] + wide[:, LANES:]
        for index in range(2):
            where = pl.ds((2 * pair + index) * inner, inner)
            image[0, where, :] = points[2 * index * inner : (2 * index + 1) * inner]
            image[1, where, :] = points[(2 * index + 1) * inner : (2 * index + 2) * inner]

    def receive_points():
        finish_exchange(out_fwd, in_fwd, fwd_send, fwd_recv)
        for pair in range(rows // 2):
            points_of_rows(pair)

    def modes_of_rows(pair, slot, factor):
        where = pl.ds(2 * pair * inner, 2 * inner)
        product = factor * (
            images[0, 0, where, :] * images[slot, 1, where, :]
            + images[slot, 0, where, :] * images[0, 1, where, :]
        )
        high, low = split(product)
        turned = dot(jnp.concatenate([high, low, high], axis=1), begin_ref[...])
        cos, sin = twist_ref[0], twist_ref[1]
        columns = []
        for index in range(2):
            part = turned[index * inner : (index + 1) * inner]
            real, imag = part[:, :LANES], part[:, LANES:]
            columns.append(
                jnp.concatenate([real * cos + imag * sin, imag * cos - real * sin], axis=0)
            )
        operand = right_operand(jnp.concatenate(columns, axis=1))
        summed = dot(scatter_ref[...], operand)
        for index in range(2):
            part = summed[:, index * LANES : (index + 1) * LANES]
            first, second = to_modes(part[:group_size], part[group_size:])
            picked = pl.ds(2 * pair + index, group_size, stride=rows)
            out_back[0, picked, :] = first
            out_back[1, picked, :] = second

    def precondition():
        per_step = 8
        for side in range(2):
            operand = right[side]

            def step(block, carry):
                base = side * half + block * per_step
                where = pl.ds(pl.multiple_of(base * degrees, degrees), per_step * degrees)
                wide = dot(tau_terms[where, :], operand)
                narrow = wide[:, :LANES] + wide[:, LANES:]
                total = applied[side]
                for index in range(per_step):
                    mine = lane % half == block * per_step + index
                    total = jnp.where(mine, narrow[index * degrees : (index + 1) * degrees], total)
                applied[side] = total
                return carry

            lax.fori_loop(0, half // per_step, step, 0)

    def by_flow(values, masks):
        low = jnp.sum(jnp.where(jnp.logical_and(masks, low_flow), values, 0.0), axis=1, keepdims=True)
        high = jnp.sum(
            jnp.where(jnp.logical_and(masks, ~low_flow), values, 0.0), axis=1, keepdims=True
        )
        return jnp.where(low_flow, low, high)

    stat_row = lax.broadcasted_iota(jnp.int32, (8, LANES), 0)
    stat_lane = lax.broadcasted_iota(jnp.int32, (8, LANES), 1) % local_modes
    packed = stat_row == stat_lane

    def send_stats(partial):
        sums = by_flow(partial, stat_row >= 0)
        out_stat[...] = jnp.sum(jnp.where(packed, sums, 0.0), axis=0, keepdims=True)

        def step(offset, carry):
            peer = lax.rem(me + offset, group_size)
            pltpu.make_async_remote_copy(
                src_ref=out_stat,
                dst_ref=in_stat.at[me],
                send_sem=stat_send,
                recv_sem=stat_recv,
                device_id=(peer // minor, lax.rem(peer, minor)),
                device_id_type=pl.DeviceIdType.MESH,
            ).start()
            return carry

        pltpu.make_async_copy(out_stat, in_stat.at[me], stat_recv).start()
        lax.fori_loop(1, group_size, step, 0)

    def receive_stats():
        sent = pl.ds(0, group_size - 1)
        pltpu.make_async_copy(in_stat.at[sent], in_stat.at[sent], stat_send).wait()
        pltpu.make_async_copy(in_stat, in_stat, stat_recv).wait()
        total = jnp.sum(in_stat[...], axis=0)
        return by_flow(jnp.broadcast_to(total, (8, LANES)), packed)

    vectors[...] = jnp.zeros_like(vectors)
    images[...] = jnp.zeros_like(images)
    vectors[0] = start_ref[...]
    send_values(start_ref[0], start_ref[1])

    chunk = stage.shape[1]
    chunks = tau_terms.shape[0] // chunk

    def fetch(index, slot):
        where = pl.ds(pl.multiple_of(index * chunk, chunk), chunk)
        return pltpu.make_async_copy(taus_ref.at[where, :], stage.at[slot], stage_sem.at[slot])

    fetch(0, 0).start()

    def load(index, carry):
        slot = lax.rem(index, 2)

        @pl.when(index + 1 < chunks)
        def _():
            fetch(index + 1, 1 - slot).start()

        fetch(index, slot).wait()
        high, low = split(stage[slot])
        where = pl.ds(pl.multiple_of(index * chunk, chunk), chunk)
        tau_terms[where, :degrees] = high
        tau_terms[where, degrees:] = low
        return carry

    lax.fori_loop(0, chunks, load, 0)

    receive_points()
    images[0] = image[...]

    def iteration(index, carry):
        phase = lax.rem(index, KRYLOV + 1)
        opening = phase == 0
        factor = jnp.where(opening, 0.5 * STRENGTH, STRENGTH)
        for pair in range(rows // 2):
            modes_of_rows(pair, phase, factor)
        exchange(out_back, in_back, back_send, back_recv)
        finish_exchange(out_back, in_back, back_send, back_recv)
        operand = right_operand(jnp.concatenate([in_back[0], in_back[1]], axis=1))
        coefs = dot(to_degrees_ref[...], operand)
        drive = jnp.where(opening, 1.0, 0.0)
        for side in range(2):
            part = coefs[:, side * LANES : (side + 1) * LANES] - drive * forcing_ref[side]
            high, low = split(part)
            both = jnp.concatenate([high, low], axis=1)
            right[side, :degrees] = both
            right[side, degrees:] = both
        precondition()
        partial = [jnp.zeros((1, LANES), jnp.float32) for _ in range(4)]
        for side in range(2):
            whole = vectors[phase, side] + applied[side]
            applied[side] = whole
            for known in range(KRYLOV):
                partial[known] += jnp.sum(vectors[known + 1, side] * whole, axis=0, keepdims=True)
            partial[KRYLOV] += jnp.sum(whole * whole, axis=0, keepdims=True)
        used = [jnp.where(known < phase, partial[known], 0.0) for known in range(KRYLOV)]
        zero = jnp.zeros((1, LANES), jnp.float32)
        send_stats(jnp.concatenate(used + [partial[KRYLOV]] + [zero] * (7 - KRYLOV), axis=0))

        @pl.when(phase < KRYLOV)
        def _():
            send_values(applied[0], applied[1])

        stats = receive_stats()
        history[phase] = stats
        inner_products = [stats[known : known + 1] for known in range(KRYLOV)]
        square = stats[KRYLOV : KRYLOV + 1]
        for value in inner_products:
            square = square - value * value
        scale = jnp.where(opening, -1.0, 1.0) / jnp.sqrt(square)

        @pl.when(phase < KRYLOV)
        def _():
            for side in range(2):
                whole = applied[side]
                for known in range(KRYLOV):
                    whole = whole - inner_products[known] * vectors[known + 1, side]
                vectors[phase + 1, side] = scale * whole
            receive_points()
            for part in range(2):
                whole = image[part]
                for known in range(KRYLOV):
                    whole = whole - inner_products[known] * images[known + 1, part]
                images[phase + 1, part] = scale * whole

        @pl.when(phase == KRYLOV)
        def _():
            hessen = []
            for column in range(KRYLOV):
                kept = history[column + 1]
                entries = [kept[known : known + 1] for known in range(column + 1)]
                length = kept[KRYLOV : KRYLOV + 1]
                for value in entries:
                    length = length - value * value
                hessen.append(jnp.stack(entries + [jnp.sqrt(length)], axis=1))
            solved = least_squares(hessen, jnp.sqrt(history[0][KRYLOV : KRYLOV + 1]))
            for side in range(2):
                whole = vectors[0, side]
                for known in range(KRYLOV):
                    whole = whole + solved[known] * vectors[known + 1, side]
                vectors[0, side] = whole
            for part in range(2):
                whole = images[0, part]
                for known in range(KRYLOV):
                    whole = whole + solved[known] * images[known + 1, part]
                images[0, part] = whole

        return carry

    lax.fori_loop(0, NEWTON * (KRYLOV + 1), iteration, 0)
    out_ref[...] = vectors[0]


def solve_flows(start, forcing, taus):
    group_size = lax.axis_size(AXES)
    minor = lax.axis_size(AXES[1])
    batch, parts, local_modes, degrees = start.shape
    rows = degrees // group_size
    inner = 2 * group_size
    half = local_modes // 2
    tables = tables_of(local_modes, group_size, degrees)
    sizes = (group_size, minor, local_modes, rows, degrees, inner)

    def pack(field):
        field = field.reshape(batch, parts, 2, half, degrees)
        return field.transpose(2, 4, 0, 1, 3).reshape(2, degrees, LANES)

    def unpack(field):
        field = field.reshape(2, degrees, batch, parts, half)
        return field.transpose(2, 3, 0, 4, 1).reshape(batch, parts, local_modes, degrees)

    field = (2, degrees, LANES)
    image = (2, rows * inner, LANES)
    chunk = 4 * degrees
    vmem = pl.BlockSpec(memory_space=pltpu.VMEM)
    out = pl.pallas_call(
        functools.partial(flow_solver, sizes),
        out_shape=jax.ShapeDtypeStruct(field, jnp.float32),
        in_specs=[vmem, vmem, pl.BlockSpec(memory_space=pl.ANY)] + [vmem] * len(tables),
        out_specs=vmem,
        scratch_shapes=[
            pltpu.VMEM((local_modes * degrees, 2 * degrees), jnp.bfloat16),
            pltpu.VMEM((2, chunk, degrees), jnp.float32),
            pltpu.VMEM((KRYLOV + 1,) + field, jnp.float32),
            pltpu.VMEM(field, jnp.float32),
            pltpu.VMEM((2, 2 * degrees, 2 * LANES), jnp.bfloat16),
            pltpu.VMEM((KRYLOV + 1,) + image, jnp.float32),
            pltpu.VMEM(image, jnp.float32),
            pltpu.VMEM(field, jnp.float32),
            pltpu.VMEM(field, jnp.float32),
            pltpu.VMEM(field, jnp.float32),
            pltpu.VMEM(field, jnp.float32),
            pltpu.VMEM((1, LANES), jnp.float32),
            pltpu.VMEM((group_size, 1, LANES), jnp.float32),
            pltpu.VMEM((KRYLOV + 1, 8, LANES), jnp.float32),
            pltpu.SemaphoreType.DMA((2,)),
        ]
        + [pltpu.SemaphoreType.DMA] * 6,
        compiler_params=pltpu.CompilerParams(
            has_side_effects=True, vmem_limit_bytes=56 * 1024 * 1024
        ),
    )(
        pack(start),
        pack(forcing * (jnp.arange(degrees) < degrees - 2).astype(jnp.float32)),
        taus.reshape(local_modes * degrees, degrees),
        *[jnp.asarray(table) for table in tables],
    )
    return unpack(out)


def fits_kernel(start):
    batch, parts, local_modes, degrees = start.shape
    rows = degrees // lax.axis_size(AXES)
    return (batch, parts, rows, batch * local_modes) == (2, 2, 8, LANES)


def local_step(start, forcing, taus):
    if fits_kernel(start):
        return solve_flows(start, forcing, taus)
    return shards(start, forcing, taus)


def solution(mesh):
    return jax.shard_map(
        local_step,
        mesh=mesh,
        in_specs=(
            P(None, None, ("modes", "cheb"), None),
            P(None, None, ("modes", "cheb"), None),
            P(("modes", "cheb"), None, None),
        ),
        out_specs=P(None, None, ("modes", "cheb"), None),
        check_vma=False,
    )
```

```python
import functools
import math

import jax
import jax.numpy as jnp
import numpy as np
from jax import lax
from jax.experimental import pallas as pl
from jax.experimental.pallas import tpu as pltpu
from jax.sharding import PartitionSpec as P

NEWTON = 2
KRYLOV = 3


PREC = lax.Precision.HIGH
STRENGTH = 0.1
AXES = ("modes", "cheb")
STAT_LANES = 128
LANES = 128


def cheb_rows(degree_count):
    degree = jnp.arange(degree_count, dtype=jnp.int32)[:, None]
    node = 2 * jnp.arange(degree_count, dtype=jnp.int32)[None, :] + 1
    turns = degree * node % (4 * degree_count)
    return jnp.cos(2.0 * math.pi / (4 * degree_count) * turns.astype(jnp.float32))


def phase_table(row_count, col_count, period):
    row_index = jnp.arange(row_count, dtype=jnp.int32)[:, None]
    col_index = jnp.arange(col_count, dtype=jnp.int32)[None, :]
    turns = row_index * col_index % period
    angle = 2.0 * math.pi / period * turns.astype(jnp.float32)
    return (jnp.cos(angle), jnp.sin(angle))


def least_squares(hessen, beta_norm):
    steps_count = len(hessen)
    matrix = [
        [hessen[col_index][:, row_index] for row_index in range(col_index + 2)]
        for col_index in range(steps_count)
    ]
    target = [beta_norm] + [jnp.zeros_like(beta_norm) for row_index in range(steps_count)]
    cosines = []
    sines_list = []
    for col_index in range(steps_count):
        column = matrix[col_index]
        for row_index in range(col_index):
            upper_entry = (
                cosines[row_index] * column[row_index]
                + sines_list[row_index] * column[row_index + 1]
            )
            lower_entry = (
                cosines[row_index] * column[row_index + 1]
                - sines_list[row_index] * column[row_index]
            )
            column[row_index] = upper_entry
            column[row_index + 1] = lower_entry
        radius = jnp.sqrt(
            column[col_index] * column[col_index] + column[col_index + 1] * column[col_index + 1]
        )
        cosines.append(column[col_index] / radius)
        sines_list.append(column[col_index + 1] / radius)
        column[col_index] = radius
        target[col_index + 1] = -sines_list[col_index] * target[col_index]
        target[col_index] = cosines[col_index] * target[col_index]
    solved = [None] * steps_count
    for row_index in reversed(range(steps_count)):
        partial_sum = target[row_index]
        for col_index in range(row_index + 1, steps_count):
            partial_sum = partial_sum - matrix[col_index][row_index] * solved[col_index]
        solved[row_index] = partial_sum / matrix[row_index][row_index]
    return solved


def shards(start, forcing, taus):
    group_size = lax.axis_size(AXES)
    batch, parts, local_modes, degrees = start.shape
    total_modes = local_modes * group_size
    points_count = 2 * total_modes
    outer_len = max(2 ** ((points_count.bit_length() - 1) // 2), local_modes)
    inner_len = points_count // outer_len
    half_inner = inner_len // 2
    split = outer_len // local_modes
    rows = degrees // group_size
    block_lanes = batch * 2 * local_modes
    fields = rows * batch
    spread = 1.0 / math.sqrt(total_modes * degrees)
    gather_factor = math.sqrt(total_modes * degrees) / points_count
    cheb_table = cheb_rows(degrees)
    tau_keep = (jnp.arange(degrees) < degrees - 2).astype(jnp.float32)
    coef_weights = jnp.where(jnp.arange(degrees) == 0, 1.0, 2.0).astype(jnp.float32) / degrees
    back_table = cheb_table * (coef_weights * tau_keep)[:, None]

    section_cos, section_sin = phase_table(inner_len, half_inner, inner_len)
    value_table = jnp.stack([section_cos, section_sin])
    slope_table = jnp.stack([-section_sin, section_cos])
    back_cos, back_sin = section_cos.T, section_sin.T
    twist_cos, twist_sin = phase_table(inner_len, outer_len, points_count)
    final_cos, final_sin = phase_table(outer_len, outer_len, outer_len)
    turn_cos = (
        twist_cos[:, :, None] * final_cos[None] - twist_sin[:, :, None] * final_sin[None]
    )
    turn_sin = (
        twist_sin[:, :, None] * final_cos[None] + twist_cos[:, :, None] * final_sin[None]
    )
    turn_table = lax.optimization_barrier(
        jnp.concatenate([turn_cos, -turn_sin, -turn_sin, -turn_cos], axis=1)
    )
    mode = (
        outer_len * jnp.arange(half_inner, dtype=jnp.int32)[:, None]
        + jnp.arange(outer_len, dtype=jnp.int32)[None, :]
    )
    paired_mode = jnp.concatenate([mode, mode], axis=1)[:, None, :]
    weights = jnp.where(paired_mode == 0, 1.0, 2.0).astype(jnp.float32) * spread
    slope_weights = weights * (16.0 * paired_mode.astype(jnp.float32) / total_modes)

    def exchange(blocks):
        return lax.all_to_all(blocks, AXES, split_axis=0, concat_axis=0, tiled=True)

    def stat_block(stats):
        flat = jnp.pad(stats.reshape(-1), (0, STAT_LANES - stats.size))
        return jnp.broadcast_to(flat, (group_size, rows, STAT_LANES))

    def read_stats(received, shape):
        flat = jnp.sum(received[:, 0, :], axis=0)
        return flat[: math.prod(shape)].reshape(shape)

    def to_points(coefs, stats):
        values = jnp.einsum("ni,brkn->ibrk", cheb_table, coefs, precision=PREC)
        blocks = values.reshape(group_size, rows, block_lanes)
        if stats is not None:
            blocks = jnp.concatenate([blocks, stat_block(stats)], axis=2)
        received = exchange(blocks)
        summed = None
        if stats is not None:
            summed = read_stats(received[:, :, block_lanes:], stats.shape)
            received = received[:, :, :block_lanes]
        spectrum = received.reshape(half_inner, split, rows, batch, 2, local_modes)
        spectrum = spectrum.transpose(0, 2, 3, 4, 1, 5).reshape(
            half_inner, fields, 2 * outer_len
        )

        def points_of(table, weighted):
            turned = jnp.einsum("sjq,qyl->jysl", table, weighted, precision=PREC)
            turned = turned.reshape(inner_len, fields, 4 * outer_len)
            return jnp.einsum("jyl,jlt->jyt", turned, turn_table, precision=PREC)

        values = points_of(value_table, spectrum * weights)
        slopes = points_of(slope_table, spectrum * slope_weights)
        return (values, slopes), summed

    def to_coefficients(points):
        turned = jnp.einsum("jyt,jlt->jyl", points, turn_table, precision=PREC) * gather_factor
        direct = turned[:, :, : 2 * outer_len].reshape(inner_len, -1)
        swapped = turned[:, :, 2 * outer_len :].reshape(inner_len, -1)
        spectrum = jnp.dot(back_cos, direct, precision=PREC) + jnp.dot(
            back_sin, swapped, precision=PREC
        )
        blocks = spectrum.reshape(half_inner, rows, batch, 2, split, local_modes)
        blocks = blocks.transpose(0, 4, 1, 2, 3, 5).reshape(group_size, rows, block_lanes)
        received = exchange(blocks).reshape(degrees, batch, 2, local_modes)
        return jnp.einsum("ibrk,ni->brkn", received, back_table, precision=PREC)

    def precondition(coefs):
        return jnp.einsum("kam,brkm->brka", taus, coefs, precision=PREC)

    def on_points(scale):
        return jnp.tile(scale, rows)[None, :, None]

    def on_coefs(scale):
        return scale[:, None, None, None]

    iterate = start
    kept_forcing = forcing * tau_keep
    base, nothing = to_points(iterate, None)
    for newton_step in range(NEWTON):
        base_points, base_slopes = base
        residual = iterate + precondition(
            to_coefficients(STRENGTH * base_points * base_slopes) - kept_forcing
        )
        local_square = jnp.sum(residual * residual, axis=(1, 2, 3))
        image, squared = to_points(residual, local_square)
        beta_norm = jnp.sqrt(squared)
        krylov_basis = [-residual / on_coefs(beta_norm)]
        images = [tuple(-part / on_points(beta_norm) for part in image)]
        hessen = []
        for column in range(KRYLOV):
            probe_points, probe_slopes = images[column]
            product = STRENGTH * (base_points * probe_slopes + probe_points * base_slopes)
            applied = krylov_basis[column] + precondition(to_coefficients(product))
            local_stats = jnp.stack(
                [jnp.sum(vector * applied, axis=(1, 2, 3)) for vector in krylov_basis + [applied]],
                axis=1,
            )
            last = column == KRYLOV - 1
            if last:
                stats = read_stats(exchange(stat_block(local_stats)), local_stats.shape)
            else:
                image, stats = to_points(applied, local_stats)
            projections, square = stats[:, :-1], stats[:, -1]
            length = jnp.sqrt(square - jnp.sum(projections * projections, axis=1))
            hessen.append(jnp.concatenate([projections, length[:, None]], axis=1))
            if not last:
                for index in range(column + 1):
                    applied = applied - on_coefs(projections[:, index]) * krylov_basis[index]
                    image = tuple(
                        part - on_points(projections[:, index]) * known
                        for part, known in zip(image, images[index])
                    )
                krylov_basis.append(applied / on_coefs(length))
                images.append(tuple(part / on_points(length) for part in image))
        solved = least_squares(hessen, beta_norm)
        for column in range(KRYLOV):
            iterate = iterate + on_coefs(solved[column]) * krylov_basis[column]
            base = tuple(
                part + on_points(solved[column]) * known
                for part, known in zip(base, images[column])
            )
    return iterate


def split_table(table):
    table = np.asarray(table, np.float32)
    high = table.astype(jnp.bfloat16)
    low = (table - high.astype(np.float32)).astype(jnp.bfloat16)
    return high, low


def left_table(table):
    high, low = split_table(table)
    return np.concatenate([high, low, high], axis=1)


def right_table(table):
    high, low = split_table(table)
    return np.concatenate([high, high, low], axis=0)


def tables_of(local_modes, group_size, degrees):
    total = local_modes * group_size
    points = 2 * total
    inner = points // local_modes
    half = local_modes // 2
    spread = 1.0 / math.sqrt(total * degrees)
    degree = np.arange(degrees)[:, None]
    node = 2 * np.arange(degrees)[None, :] + 1
    cheb = np.cos(2.0 * np.pi / (4 * degrees) * (degree * node % (4 * degrees)))
    coef_weights = np.where(np.arange(degrees) == 0, 1.0, 2.0) / degrees
    keep = np.arange(degrees) < degrees - 2
    to_rows = left_table(cheb.T)
    to_degrees = right_table(cheb * (coef_weights * keep)[:, None])

    j_low = np.arange(inner)[:, None]
    source = np.arange(group_size)[None, :]
    angle = 2.0 * np.pi / inner * (j_low * source % inner)
    cos, sin = np.cos(angle), np.sin(angle)
    real = np.concatenate([cos, -sin], axis=1)
    imag = np.concatenate([sin, cos], axis=1)
    wave = np.tile(16.0 * local_modes * source / total, (1, 2))
    gather = 2.0 * spread * np.concatenate([real, imag, real * wave, imag * wave], axis=0)
    gather = left_table(gather)
    scatter = np.concatenate(
        [np.concatenate([cos.T, sin.T], axis=1), np.concatenate([-sin.T, cos.T], axis=1)], axis=0
    )
    scatter = left_table(scatter * math.sqrt(total * degrees) / points)

    lane_mode = np.tile(np.arange(local_modes), 2)[None, :]
    twist = 2.0 * np.pi / points * (j_low * lane_mode)
    wave_low = np.broadcast_to(16.0 * lane_mode / total, twist.shape)
    twist = np.stack([np.cos(twist), np.sin(twist), wave_low]).astype(np.float32)

    mode = np.arange(local_modes)
    final = 2.0 * np.pi / local_modes * (mode[:, None] * mode[None, :] % local_modes)
    pair = np.eye(2)
    cos_high, cos_low = split_table(np.kron(pair, np.cos(final)))
    sin_high, sin_low = split_table(np.kron(pair, np.sin(final)))
    cos_row = np.concatenate([cos_high, cos_low], axis=1)
    sin_row = np.concatenate([-sin_high, -sin_low], axis=1)
    finish = np.concatenate([cos_row, sin_row, cos_row, sin_row], axis=0)
    high_row = np.concatenate([cos_high, -sin_high], axis=1)
    low_row = np.concatenate([cos_low, -sin_low], axis=1)
    begin = np.concatenate([high_row, high_row, low_row], axis=0)
    return to_rows, to_degrees, gather, scatter, twist, finish, begin


def split(value):
    high = value.astype(jnp.bfloat16)
    return high, (value - high.astype(jnp.float32)).astype(jnp.bfloat16)


def right_operand(value):
    high, low = split(value)
    return jnp.concatenate([high, high, low], axis=0)


def dot(left, right):
    return jnp.dot(left, right, preferred_element_type=jnp.float32)


def flow_solver(
    sizes,
    start_ref,
    forcing_ref,
    taus_ref,
    to_rows_ref,
    to_degrees_ref,
    gather_ref,
    scatter_ref,
    twist_ref,
    finish_ref,
    begin_ref,
    out_ref,
    tau_terms,
    stage,
    vectors,
    applied,
    partial,
    driven,
    images,
    image,
    out_fwd,
    in_fwd,
    out_back,
    in_back,
    out_stat,
    in_stat,
    history,
    stage_sem,
    fwd_send,
    fwd_recv,
    back_send,
    back_recv,
    stat_send,
    stat_recv,
):
    group_size, minor, local_modes, rows, degrees, inner = sizes
    half = local_modes // 2
    per_dot = 4
    me = lax.axis_index(AXES[0]) * minor + lax.axis_index(AXES[1])
    lane = lax.broadcasted_iota(jnp.int32, (1, LANES), 1)
    first_half = lane % local_modes < half
    low_flow = lane < local_modes

    def own_rows(index):
        return pl.ds(pl.multiple_of(index * rows, rows), rows)

    flips = []
    for bit in range(group_size.bit_length() - 1):
        flips.append((1 << bit) - (2 << bit) * lax.rem(me // (1 << bit), 2))

    def peers():
        for distance in reversed(range(1, group_size)):
            peer = me
            for bit, flip in enumerate(flips):
                if distance >> bit & 1:
                    peer = peer + flip
            yield peer, (peer // minor, lax.rem(peer, minor))

    def exchange(src, dst, send_sem, recv_sem):
        for peer, place in peers():
            pltpu.make_async_remote_copy(
                src_ref=src.at[own_rows(peer), :],
                dst_ref=dst.at[own_rows(me), :],
                send_sem=send_sem,
                recv_sem=recv_sem,
                device_id=place,
                device_id_type=pl.DeviceIdType.MESH,
            ).start()
        pltpu.make_async_copy(
            src.at[own_rows(me), :], dst.at[own_rows(me), :], recv_sem
        ).start()

    def finish_exchange(src, dst, send_sem, recv_sem):
        sent = pl.ds(0, (group_size - 1) * rows)
        pltpu.make_async_copy(src.at[sent, :], dst.at[sent, :], send_sem).wait()
        pltpu.make_async_copy(src, dst, recv_sem).wait()

    def to_modes(first, second):
        turned = pltpu.roll(second, half, 1)
        back = pltpu.roll(first, LANES - half, 1)
        return jnp.where(first_half, first, turned), jnp.where(first_half, back, second)

    def send_values(side, field):
        values = dot(to_rows_ref[...], right_operand(field))
        constant = jnp.logical_and(me + side == 0, lane % half == 0)
        out_fwd[side] = values * jnp.where(constant, 0.5, 1.0)
        exchange(out_fwd.at[side], in_fwd.at[side], fwd_send.at[side], fwd_recv.at[side])

    def points_of_rows(pair):
        columns = []
        for row in (2 * pair, 2 * pair + 1):
            picked = pl.ds(row, group_size, stride=rows)
            real, imag = to_modes(in_fwd[0, picked, :], in_fwd[1, picked, :])
            columns.append(jnp.concatenate([real, imag], axis=0))
        operand = right_operand(jnp.concatenate(columns, axis=1))
        summed = dot(gather_ref[...], operand)
        cos, sin, low = twist_ref[0], twist_ref[1], twist_ref[2]
        lefts = []
        for index in range(2):
            part = summed[:, index * LANES : (index + 1) * LANES]
            real, imag, wave_real, wave_imag = (
                part[n * inner : (n + 1) * inner] for n in range(4)
            )
            slope_real = -(wave_imag + low * imag)
            slope_imag = wave_real + low * real
            for re, im in ((real, imag), (slope_real, slope_imag)):
                re_high, re_low = split(re * cos - im * sin)
                im_high, im_low = split(re * sin + im * cos)
                lefts.append(jnp.concatenate([re_high, im_high, re_low, im_low], axis=1))
        wide = dot(jnp.concatenate(lefts, axis=0), finish_ref[...])
        points = wide[:, :LANES] + wide[:, LANES:]
        for index in range(2):
            where = pl.ds((2 * pair + index) * inner, inner)
            image[0, where, :] = points[2 * index * inner : (2 * index + 1) * inner]
            image[1, where, :] = points[(2 * index + 1) * inner : (2 * index + 2) * inner]

    def receive_points():
        for side in range(2):
            finish_exchange(
                out_fwd.at[side], in_fwd.at[side], fwd_send.at[side], fwd_recv.at[side]
            )
        for pair in range(rows // 2):
            points_of_rows(pair)

    def modes_of_rows(pair, slot, factor):
        where = pl.ds(2 * pair * inner, 2 * inner)
        product = factor * (
            images[0, 0, where, :] * images[slot, 1, where, :]
            + images[slot, 0, where, :] * images[0, 1, where, :]
        )
        high, low = split(product)
        turned = dot(jnp.concatenate([high, low, high], axis=1), begin_ref[...])
        cos, sin = twist_ref[0], twist_ref[1]
        columns = []
        for index in range(2):
            part = turned[index * inner : (index + 1) * inner]
            real, imag = part[:, :LANES], part[:, LANES:]
            columns.append(
                jnp.concatenate([real * cos + imag * sin, imag * cos - real * sin], axis=0)
            )
        operand = right_operand(jnp.concatenate(columns, axis=1))
        summed = dot(scatter_ref[...], operand)
        for index in range(2):
            part = summed[:, index * LANES : (index + 1) * LANES]
            first, second = to_modes(part[:group_size], part[group_size:])
            picked = pl.ds(2 * pair + index, group_size, stride=rows)
            out_back[0, picked, :] = first
            out_back[1, picked, :] = second

    def precondition(side, operand):
        for block in range(half // per_dot):
            base = side * half + block * per_dot
            where = pl.ds(pl.multiple_of(base * degrees, degrees), per_dot * degrees)
            wide = dot(tau_terms[where, :], operand)
            narrow = wide[:, :LANES] + wide[:, LANES:]
            total = applied[side]
            for index in range(per_dot):
                mine = lane % half == block * per_dot + index
                total = jnp.where(mine, narrow[index * degrees : (index + 1) * degrees], total)
            applied[side] = total

    def by_flow(values, masks):
        low = jnp.sum(jnp.where(jnp.logical_and(masks, low_flow), values, 0.0), axis=1, keepdims=True)
        high = jnp.sum(
            jnp.where(jnp.logical_and(masks, ~low_flow), values, 0.0), axis=1, keepdims=True
        )
        return jnp.where(low_flow, low, high)

    stat_row = lax.broadcasted_iota(jnp.int32, (8, LANES), 0)
    stat_lane = lax.broadcasted_iota(jnp.int32, (8, LANES), 1) % local_modes
    packed = stat_row == stat_lane

    def send_stats(partial):
        sums = by_flow(partial, stat_row >= 0)
        out_stat[...] = jnp.sum(jnp.where(packed, sums, 0.0), axis=0, keepdims=True)

        for peer, place in peers():
            pltpu.make_async_remote_copy(
                src_ref=out_stat,
                dst_ref=in_stat.at[me],
                send_sem=stat_send,
                recv_sem=stat_recv,
                device_id=place,
                device_id_type=pl.DeviceIdType.MESH,
            ).start()
        pltpu.make_async_copy(out_stat, in_stat.at[me], stat_recv).start()

    def receive_stats():
        sent = pl.ds(0, group_size - 1)
        pltpu.make_async_copy(in_stat.at[sent], in_stat.at[sent], stat_send).wait()
        pltpu.make_async_copy(in_stat, in_stat, stat_recv).wait()
        total = jnp.sum(in_stat[...], axis=0)
        return by_flow(jnp.broadcast_to(total, (8, LANES)), packed)

    vectors[...] = jnp.zeros_like(vectors)
    images[...] = jnp.zeros_like(images)
    vectors[0] = start_ref[...]
    for side in range(2):
        send_values(side, start_ref[side])
        driven[side] = dot(to_rows_ref[...], right_operand(forcing_ref[side]))

    chunk = stage.shape[1]
    chunks = tau_terms.shape[0] // chunk

    def fetch(index, slot):
        where = pl.ds(pl.multiple_of(index * chunk, chunk), chunk)
        return pltpu.make_async_copy(taus_ref.at[where, :], stage.at[slot], stage_sem.at[slot])

    def load(index, carry):
        slot = lax.rem(index, 2)

        @pl.when(index + 1 < chunks)
        def _():
            fetch(index + 1, 1 - slot).start()

        fetch(index, slot).wait()
        high, low = split(stage[slot])
        combined = dot(jnp.concatenate([high, low, high], axis=1), to_degrees_ref[...])
        high, low = split(combined)
        where = pl.ds(pl.multiple_of(index * chunk, chunk), chunk)
        tau_terms[where, :degrees] = high
        tau_terms[where, degrees:] = low
        return carry

    fetch(0, 0).start()
    lax.fori_loop(0, chunks // 2, load, 0)

    receive_points()
    images[0] = image[...]

    def iteration(index, carry):
        phase = lax.rem(index, KRYLOV + 1)
        opening = phase == 0
        factor = jnp.where(opening, 0.5 * STRENGTH, STRENGTH)
        for pair in range(rows // 2):
            modes_of_rows(pair, phase, factor)
        for side in range(2):
            exchange(out_back.at[side], in_back.at[side], back_send.at[side], back_recv.at[side])

        @pl.when(index == 0)
        def _():
            lax.fori_loop(chunks // 2, chunks, load, 0)

        drive = jnp.where(opening, 1.0, 0.0)
        partial[...] = jnp.zeros_like(partial)

        def half_step(side, carry):
            finish_exchange(
                out_back.at[side], in_back.at[side], back_send.at[side], back_recv.at[side]
            )
            high, low = split(in_back[side] - drive * driven[side])
            both = jnp.concatenate([high, low], axis=1)
            precondition(side, jnp.concatenate([both, both], axis=0))
            whole = vectors[phase, side] + applied[side]
            applied[side] = whole
            sums = [
                jnp.sum(vectors[known + 1, side] * whole, axis=0, keepdims=True)
                for known in range(KRYLOV)
            ]
            sums = [jnp.where(known < phase, sums[known], 0.0) for known in range(KRYLOV)]
            sums.append(jnp.sum(whole * whole, axis=0, keepdims=True))
            sums += [jnp.zeros((1, LANES), jnp.float32)] * (7 - KRYLOV)
            partial[...] += jnp.concatenate(sums, axis=0)

            @pl.when(side == 1)
            def _():
                send_stats(partial[...])

            @pl.when(phase < KRYLOV)
            def _():
                send_values(side, applied[side])

            return carry

        lax.fori_loop(0, 2, half_step, 0)
        stats = receive_stats()
        history[phase] = stats
        inner_products = [stats[known : known + 1] for known in range(KRYLOV)]
        square = stats[KRYLOV : KRYLOV + 1]
        for value in inner_products:
            square = square - value * value
        scale = jnp.where(opening, -1.0, 1.0) / jnp.sqrt(square)

        @pl.when(phase < KRYLOV)
        def _():
            for side in range(2):
                whole = applied[side]
                for known in range(KRYLOV):
                    whole = whole - inner_products[known] * vectors[known + 1, side]
                vectors[phase + 1, side] = scale * whole
            receive_points()
            for part in range(2):
                whole = image[part]
                for known in range(KRYLOV):
                    whole = whole - inner_products[known] * images[known + 1, part]
                images[phase + 1, part] = scale * whole

        @pl.when(phase == KRYLOV)
        def _():
            hessen = []
            for column in range(KRYLOV):
                kept = history[column + 1]
                entries = [kept[known : known + 1] for known in range(column + 1)]
                length = kept[KRYLOV : KRYLOV + 1]
                for value in entries:
                    length = length - value * value
                hessen.append(jnp.stack(entries + [jnp.sqrt(length)], axis=1))
            solved = least_squares(hessen, jnp.sqrt(history[0][KRYLOV : KRYLOV + 1]))
            for side in range(2):
                whole = vectors[0, side]
                for known in range(KRYLOV):
                    whole = whole + solved[known] * vectors[known + 1, side]
                vectors[0, side] = whole
            for part in range(2):
                whole = images[0, part]
                for known in range(KRYLOV):
                    whole = whole + solved[known] * images[known + 1, part]
                images[0, part] = whole

        return carry

    lax.fori_loop(0, NEWTON * (KRYLOV + 1), iteration, 0)
    out_ref[...] = vectors[0]


def solve_flows(start, forcing, taus):
    group_size = lax.axis_size(AXES)
    minor = lax.axis_size(AXES[1])
    batch, parts, local_modes, degrees = start.shape
    rows = degrees // group_size
    inner = 2 * group_size
    half = local_modes // 2
    tables = tables_of(local_modes, group_size, degrees)
    sizes = (group_size, minor, local_modes, rows, degrees, inner)

    def pack(field):
        field = field.reshape(batch, parts, 2, half, degrees)
        return field.transpose(2, 4, 0, 1, 3).reshape(2, degrees, LANES)

    def unpack(field):
        field = field.reshape(2, degrees, batch, parts, half)
        return field.transpose(2, 3, 0, 4, 1).reshape(batch, parts, local_modes, degrees)

    field = (2, degrees, LANES)
    image = (2, rows * inner, LANES)
    chunk = 4 * degrees
    vmem = pl.BlockSpec(memory_space=pltpu.VMEM)
    out = pl.pallas_call(
        functools.partial(flow_solver, sizes),
        out_shape=jax.ShapeDtypeStruct(field, jnp.float32),
        in_specs=[vmem, vmem, pl.BlockSpec(memory_space=pl.ANY)] + [vmem] * len(tables),
        out_specs=vmem,
        scratch_shapes=[
            pltpu.VMEM((local_modes * degrees, 2 * degrees), jnp.bfloat16),
            pltpu.VMEM((2, chunk, degrees), jnp.float32),
            pltpu.VMEM((KRYLOV + 1,) + field, jnp.float32),
            pltpu.VMEM(field, jnp.float32),
            pltpu.VMEM((8, LANES), jnp.float32),
            pltpu.VMEM(field, jnp.float32),
            pltpu.VMEM((KRYLOV + 1,) + image, jnp.float32),
            pltpu.VMEM(image, jnp.float32),
            pltpu.VMEM(field, jnp.float32),
            pltpu.VMEM(field, jnp.float32),
            pltpu.VMEM(field, jnp.float32),
            pltpu.VMEM(field, jnp.float32),
            pltpu.VMEM((1, LANES), jnp.float32),
            pltpu.VMEM((group_size, 1, LANES), jnp.float32),
            pltpu.VMEM((KRYLOV + 1, 8, LANES), jnp.float32),
            pltpu.SemaphoreType.DMA((2,)),
        ]
        + [pltpu.SemaphoreType.DMA((2,))] * 4
        + [pltpu.SemaphoreType.DMA] * 2,
        compiler_params=pltpu.CompilerParams(
            has_side_effects=True, vmem_limit_bytes=56 * 1024 * 1024
        ),
    )(
        pack(start),
        pack(forcing),
        taus.reshape(local_modes * degrees, degrees),
        *[jnp.asarray(table) for table in tables],
    )
    return unpack(out)


def fits_kernel(start):
    batch, parts, local_modes, degrees = start.shape
    group = lax.axis_size(AXES)
    rows = degrees // group
    fits = (batch, parts, rows, batch * local_modes) == (2, 2, 8, LANES)
    return fits and group & (group - 1) == 0


def local_step(start, forcing, taus):
    if fits_kernel(start):
        return solve_flows(start, forcing, taus)
    return shards(start, forcing, taus)


def solution(mesh):
    return jax.shard_map(
        local_step,
        mesh=mesh,
        in_specs=(
            P(None, None, ("modes", "cheb"), None),
            P(None, None, ("modes", "cheb"), None),
            P(("modes", "cheb"), None, None),
        ),
        out_specs=P(None, None, ("modes", "cheb"), None),
        check_vma=False,
    )
```

```python
import functools
import math

import jax
import jax.numpy as jnp
import numpy as np
from jax import lax
from jax.experimental import pallas as pl
from jax.experimental.pallas import tpu as pltpu
from jax.sharding import PartitionSpec as P

NEWTON = 2
KRYLOV = 3


PREC = lax.Precision.HIGH
STRENGTH = 0.1
AXES = ("modes", "cheb")
STAT_LANES = 128
LANES = 128


def cheb_rows(degree_count):
    degree = jnp.arange(degree_count, dtype=jnp.int32)[:, None]
    node = 2 * jnp.arange(degree_count, dtype=jnp.int32)[None, :] + 1
    turns = degree * node % (4 * degree_count)
    return jnp.cos(2.0 * math.pi / (4 * degree_count) * turns.astype(jnp.float32))


def phase_table(row_count, col_count, period):
    row_index = jnp.arange(row_count, dtype=jnp.int32)[:, None]
    col_index = jnp.arange(col_count, dtype=jnp.int32)[None, :]
    turns = row_index * col_index % period
    angle = 2.0 * math.pi / period * turns.astype(jnp.float32)
    return (jnp.cos(angle), jnp.sin(angle))


def least_squares(matrix, beta_norm):
    steps_count = len(matrix)
    target = [beta_norm] + [jnp.zeros_like(beta_norm) for row_index in range(steps_count)]
    cosines = []
    sines_list = []
    for col_index in range(steps_count):
        column = matrix[col_index]
        for row_index in range(col_index):
            upper_entry = (
                cosines[row_index] * column[row_index]
                + sines_list[row_index] * column[row_index + 1]
            )
            lower_entry = (
                cosines[row_index] * column[row_index + 1]
                - sines_list[row_index] * column[row_index]
            )
            column[row_index] = upper_entry
            column[row_index + 1] = lower_entry
        radius = jnp.sqrt(
            column[col_index] * column[col_index] + column[col_index + 1] * column[col_index + 1]
        )
        cosines.append(column[col_index] / radius)
        sines_list.append(column[col_index + 1] / radius)
        column[col_index] = radius
        target[col_index + 1] = -sines_list[col_index] * target[col_index]
        target[col_index] = cosines[col_index] * target[col_index]
    solved = [None] * steps_count
    for row_index in reversed(range(steps_count)):
        partial_sum = target[row_index]
        for col_index in range(row_index + 1, steps_count):
            partial_sum = partial_sum - matrix[col_index][row_index] * solved[col_index]
        solved[row_index] = partial_sum / matrix[row_index][row_index]
    return solved


def shards(start, forcing, taus):
    group_size = lax.axis_size(AXES)
    batch, parts, local_modes, degrees = start.shape
    total_modes = local_modes * group_size
    points_count = 2 * total_modes
    outer_len = max(2 ** ((points_count.bit_length() - 1) // 2), local_modes)
    inner_len = points_count // outer_len
    half_inner = inner_len // 2
    split = outer_len // local_modes
    rows = degrees // group_size
    block_lanes = batch * 2 * local_modes
    fields = rows * batch
    spread = 1.0 / math.sqrt(total_modes * degrees)
    gather_factor = math.sqrt(total_modes * degrees) / points_count
    cheb_table = cheb_rows(degrees)
    tau_keep = (jnp.arange(degrees) < degrees - 2).astype(jnp.float32)
    coef_weights = jnp.where(jnp.arange(degrees) == 0, 1.0, 2.0).astype(jnp.float32) / degrees
    back_table = cheb_table * (coef_weights * tau_keep)[:, None]

    section_cos, section_sin = phase_table(inner_len, half_inner, inner_len)
    value_table = jnp.stack([section_cos, section_sin])
    slope_table = jnp.stack([-section_sin, section_cos])
    back_cos, back_sin = section_cos.T, section_sin.T
    twist_cos, twist_sin = phase_table(inner_len, outer_len, points_count)
    final_cos, final_sin = phase_table(outer_len, outer_len, outer_len)
    turn_cos = (
        twist_cos[:, :, None] * final_cos[None] - twist_sin[:, :, None] * final_sin[None]
    )
    turn_sin = (
        twist_sin[:, :, None] * final_cos[None] + twist_cos[:, :, None] * final_sin[None]
    )
    turn_table = lax.optimization_barrier(
        jnp.concatenate([turn_cos, -turn_sin, -turn_sin, -turn_cos], axis=1)
    )
    mode = (
        outer_len * jnp.arange(half_inner, dtype=jnp.int32)[:, None]
        + jnp.arange(outer_len, dtype=jnp.int32)[None, :]
    )
    paired_mode = jnp.concatenate([mode, mode], axis=1)[:, None, :]
    weights = jnp.where(paired_mode == 0, 1.0, 2.0).astype(jnp.float32) * spread
    slope_weights = weights * (16.0 * paired_mode.astype(jnp.float32) / total_modes)

    def exchange(blocks):
        return lax.all_to_all(blocks, AXES, split_axis=0, concat_axis=0, tiled=True)

    def stat_block(stats):
        flat = jnp.pad(stats.reshape(-1), (0, STAT_LANES - stats.size))
        return jnp.broadcast_to(flat, (group_size, rows, STAT_LANES))

    def read_stats(received, shape):
        flat = jnp.sum(received[:, 0, :], axis=0)
        return flat[: math.prod(shape)].reshape(shape)

    def to_points(coefs, stats):
        values = jnp.einsum("ni,brkn->ibrk", cheb_table, coefs, precision=PREC)
        blocks = values.reshape(group_size, rows, block_lanes)
        if stats is not None:
            blocks = jnp.concatenate([blocks, stat_block(stats)], axis=2)
        received = exchange(blocks)
        summed = None
        if stats is not None:
            summed = read_stats(received[:, :, block_lanes:], stats.shape)
            received = received[:, :, :block_lanes]
        spectrum = received.reshape(half_inner, split, rows, batch, 2, local_modes)
        spectrum = spectrum.transpose(0, 2, 3, 4, 1, 5).reshape(
            half_inner, fields, 2 * outer_len
        )

        def points_of(table, weighted):
            turned = jnp.einsum("sjq,qyl->jysl", table, weighted, precision=PREC)
            turned = turned.reshape(inner_len, fields, 4 * outer_len)
            return jnp.einsum("jyl,jlt->jyt", turned, turn_table, precision=PREC)

        values = points_of(value_table, spectrum * weights)
        slopes = points_of(slope_table, spectrum * slope_weights)
        return (values, slopes), summed

    def to_coefficients(points):
        turned = jnp.einsum("jyt,jlt->jyl", points, turn_table, precision=PREC) * gather_factor
        direct = turned[:, :, : 2 * outer_len].reshape(inner_len, -1)
        swapped = turned[:, :, 2 * outer_len :].reshape(inner_len, -1)
        spectrum = jnp.dot(back_cos, direct, precision=PREC) + jnp.dot(
            back_sin, swapped, precision=PREC
        )
        blocks = spectrum.reshape(half_inner, rows, batch, 2, split, local_modes)
        blocks = blocks.transpose(0, 4, 1, 2, 3, 5).reshape(group_size, rows, block_lanes)
        received = exchange(blocks).reshape(degrees, batch, 2, local_modes)
        return jnp.einsum("ibrk,ni->brkn", received, back_table, precision=PREC)

    def precondition(coefs):
        return jnp.einsum("kam,brkm->brka", taus, coefs, precision=PREC)

    def on_points(scale):
        return jnp.tile(scale, rows)[None, :, None]

    def on_coefs(scale):
        return scale[:, None, None, None]

    iterate = start
    kept_forcing = forcing * tau_keep
    base, nothing = to_points(iterate, None)
    for newton_step in range(NEWTON):
        base_points, base_slopes = base
        residual = iterate + precondition(
            to_coefficients(STRENGTH * base_points * base_slopes) - kept_forcing
        )
        local_square = jnp.sum(residual * residual, axis=(1, 2, 3))
        image, squared = to_points(residual, local_square)
        beta_norm = jnp.sqrt(squared)
        krylov_basis = [-residual / on_coefs(beta_norm)]
        images = [tuple(-part / on_points(beta_norm) for part in image)]
        hessen = []
        for column in range(KRYLOV):
            probe_points, probe_slopes = images[column]
            product = STRENGTH * (base_points * probe_slopes + probe_points * base_slopes)
            applied = krylov_basis[column] + precondition(to_coefficients(product))
            local_stats = jnp.stack(
                [jnp.sum(vector * applied, axis=(1, 2, 3)) for vector in krylov_basis + [applied]],
                axis=1,
            )
            last = column == KRYLOV - 1
            if last:
                stats = read_stats(exchange(stat_block(local_stats)), local_stats.shape)
            else:
                image, stats = to_points(applied, local_stats)
            projections, square = stats[:, :-1], stats[:, -1]
            length = jnp.sqrt(square - jnp.sum(projections * projections, axis=1))
            hessen.append(jnp.concatenate([projections, length[:, None]], axis=1))
            if not last:
                for index in range(column + 1):
                    applied = applied - on_coefs(projections[:, index]) * krylov_basis[index]
                    image = tuple(
                        part - on_points(projections[:, index]) * known
                        for part, known in zip(image, images[index])
                    )
                krylov_basis.append(applied / on_coefs(length))
                images.append(tuple(part / on_points(length) for part in image))
        matrix = [
            [hessen[column][:, row] for row in range(column + 2)] for column in range(KRYLOV)
        ]
        solved = least_squares(matrix, beta_norm)
        for column in range(KRYLOV):
            iterate = iterate + on_coefs(solved[column]) * krylov_basis[column]
            base = tuple(
                part + on_points(solved[column]) * known
                for part, known in zip(base, images[column])
            )
    return iterate


def split_table(table):
    table = np.asarray(table, np.float32)
    high = table.astype(jnp.bfloat16)
    low = (table - high.astype(np.float32)).astype(jnp.bfloat16)
    return high, low


def left_table(table):
    high, low = split_table(table)
    return np.concatenate([high, low, high], axis=1)


def tables_of(local_modes, group_size, degrees):
    total = local_modes * group_size
    points = 2 * total
    inner = points // local_modes
    half = local_modes // 2
    spread = 1.0 / math.sqrt(total * degrees)
    degree = np.arange(degrees)[:, None]
    node = 2 * np.arange(degrees)[None, :] + 1
    cheb = np.cos(2.0 * np.pi / (4 * degrees) * (degree * node % (4 * degrees)))
    coef_weights = np.where(np.arange(degrees) == 0, 1.0, 2.0) / degrees
    keep = np.arange(degrees) < degrees - 2
    to_rows = left_table(cheb.T)
    to_degrees = left_table((cheb * (coef_weights * keep)[:, None]).T)

    j_low = np.arange(inner)[:, None]
    source = np.arange(group_size)[None, :]
    angle = 2.0 * np.pi / inner * (j_low * source % inner)
    cos, sin = np.cos(angle), np.sin(angle)
    real = np.concatenate([cos, -sin], axis=1)
    imag = np.concatenate([sin, cos], axis=1)
    wave = np.tile(16.0 * local_modes * source / total, (1, 2))
    gather = 2.0 * spread * np.concatenate([real, imag, real * wave, imag * wave], axis=0)
    gather = left_table(gather)
    scatter = np.concatenate(
        [np.concatenate([cos.T, sin.T], axis=1), np.concatenate([-sin.T, cos.T], axis=1)], axis=0
    )
    scatter = left_table(scatter * math.sqrt(total * degrees) / points)

    lane = np.arange(2 * local_modes)
    lane_mode = (lane // 4 + half * (lane % 2))[None, :]
    lane_flow = lane // 2 % 2
    twist = 2.0 * np.pi / points * (j_low * lane_mode)
    wave_low = np.broadcast_to(16.0 * lane_mode / total, twist.shape)
    twist = np.stack([np.cos(twist), np.sin(twist), wave_low]).astype(np.float32)

    final = lane_mode.T * np.tile(np.arange(local_modes), 2)[None, :] % local_modes
    final = 2.0 * np.pi / local_modes * final
    same = lane_flow[:, None] == lane[None, :] // local_modes
    cos_high, cos_low = split_table(same * np.cos(final))
    sin_high, sin_low = split_table(same * np.sin(final))
    cos_row = np.concatenate([cos_high, cos_low], axis=1)
    sin_row = np.concatenate([-sin_high, -sin_low], axis=1)
    finish = np.concatenate([cos_row, sin_row, cos_row, sin_row], axis=0)
    high_row = np.concatenate([cos_high.T, -sin_high.T], axis=1)
    low_row = np.concatenate([cos_low.T, -sin_low.T], axis=1)
    begin = np.concatenate([high_row, high_row, low_row], axis=0)
    return to_rows, to_degrees, gather, scatter, twist, finish, begin


def split(value):
    high = value.astype(jnp.bfloat16)
    return high, (value - high.astype(jnp.float32)).astype(jnp.bfloat16)


def right_operand(value):
    high, low = split(value)
    return jnp.concatenate([high, high, low], axis=0)


def dot(left, right):
    return jnp.dot(left, right, preferred_element_type=jnp.float32)


def dot_rows(left, right):
    dims = (((1,), (1,)), ((), ()))
    return lax.dot_general(left, right, dims, preferred_element_type=jnp.float32)


def row_operand(value):
    high, low = split(value)
    return jnp.concatenate([high, high, low], axis=1)


def flow_solver(
    sizes,
    start_ref,
    forcing_ref,
    taus_ref,
    to_rows_ref,
    to_degrees_ref,
    gather_ref,
    scatter_ref,
    twist_ref,
    finish_ref,
    begin_ref,
    out_ref,
    tau_terms,
    stage,
    vectors,
    applied,
    partial,
    driven,
    images,
    ordered,
    summed,
    lefts,
    products,
    rights,
    out_fwd,
    in_fwd,
    out_back,
    in_back,
    out_stat,
    in_stat,
    history,
    stage_sem,
    fwd_send,
    fwd_recv,
    back_send,
    back_recv,
    stat_send,
    stat_recv,
):
    group_size, minor, local_modes, rows, degrees, inner = sizes
    half = local_modes // 2
    me = lax.axis_index(AXES[0]) * minor + lax.axis_index(AXES[1])
    lane = lax.broadcasted_iota(jnp.int32, (1, LANES), 1)
    even_lane = lane % 2 == 0
    low_flow = lane < local_modes
    low_rows = lax.broadcasted_iota(jnp.int32, (8, LANES), 0) % 4 < 2

    def own_rows(index):
        return pl.ds(pl.multiple_of(index * rows, rows), rows)

    flips = []
    for bit in range(group_size.bit_length() - 1):
        flips.append((1 << bit) - (2 << bit) * lax.rem(me // (1 << bit), 2))

    def peers():
        for distance in reversed(range(1, group_size)):
            peer = me
            for bit, flip in enumerate(flips):
                if distance >> bit & 1:
                    peer = peer + flip
            yield peer, (peer // minor, lax.rem(peer, minor))

    def exchange(src, dst, send_sem, recv_sem):
        for peer, place in peers():
            pltpu.make_async_remote_copy(
                src_ref=src.at[own_rows(peer), :],
                dst_ref=dst.at[own_rows(me), :],
                send_sem=send_sem,
                recv_sem=recv_sem,
                device_id=place,
                device_id_type=pl.DeviceIdType.MESH,
            ).start()
        pltpu.make_async_copy(
            src.at[own_rows(me), :], dst.at[own_rows(me), :], recv_sem
        ).start()

    def finish_exchange(src, dst, send_sem, recv_sem):
        sent = pl.ds(0, (group_size - 1) * rows)
        pltpu.make_async_copy(src.at[sent, :], dst.at[sent, :], send_sem).wait()
        pltpu.make_async_copy(src, dst, recv_sem).wait()

    def to_modes(first, second):
        turned = pltpu.roll(second, 1, 1)
        back = pltpu.roll(first, LANES - 1, 1)
        return jnp.where(even_lane, first, turned), jnp.where(even_lane, back, second)

    def rows_of(field):
        return dot_rows(to_rows_ref[...], row_operand(field.reshape(LANES, degrees)))

    def send_values(side, field):
        constant = jnp.logical_and(me + side == 0, lane < 4)
        out_fwd[side] = rows_of(field) * jnp.where(constant, 0.5, 1.0)
        exchange(out_fwd.at[side], in_fwd.at[side], fwd_send.at[side], fwd_recv.at[side])

    pairs = range(rows // 2)

    def sums_over_sources():
        for pair in pairs:
            columns = []
            for row in (2 * pair, 2 * pair + 1):
                picked = pl.ds(row, group_size, stride=rows)
                real, imag = to_modes(in_fwd[0, picked, :], in_fwd[1, picked, :])
                columns.append(jnp.concatenate([real, imag], axis=0))
            operand = right_operand(jnp.concatenate(columns, axis=1))
            summed[pair] = dot(gather_ref[...], operand)
        cos, sin, low = twist_ref[0], twist_ref[1], twist_ref[2]
        for row in range(rows):
            pair, index = divmod(row, 2)
            lanes = slice(index * LANES, (index + 1) * LANES)
            real, imag, wave_real, wave_imag = (
                summed[pair, n * inner : (n + 1) * inner, lanes] for n in range(4)
            )
            slope_real = -(wave_imag + low * imag)
            slope_imag = wave_real + low * real
            for part, (re, im) in enumerate(((real, imag), (slope_real, slope_imag))):
                re_high, re_low = split(re * cos - im * sin)
                im_high, im_low = split(re * sin + im * cos)
                where = slice((2 * part + index) * inner, (2 * part + index + 1) * inner)
                lefts[pair, where] = jnp.concatenate([re_high, im_high, re_low, im_low], axis=1)

    def points_of_rows(pair):
        wide = dot(lefts[pair], finish_ref[...])
        points = wide[:, :LANES] + wide[:, LANES:]
        return points[: 2 * inner], points[2 * inner :]

    def receive_points():
        for side in range(2):
            finish_exchange(
                out_fwd.at[side], in_fwd.at[side], fwd_send.at[side], fwd_recv.at[side]
            )
        sums_over_sources()

    def pair_rows(pair):
        return pl.ds(2 * pair * inner, 2 * inner)

    def keep_product(pair, product):
        high, low = split(product)
        products[pair] = jnp.concatenate([high, low, high], axis=1)

    def send_products():
        cos, sin = twist_ref[0], twist_ref[1]
        for pair in pairs:
            turned = dot(products[pair], begin_ref[...])
            columns = []
            for index in range(2):
                part = turned[index * inner : (index + 1) * inner]
                real, imag = part[:, :LANES], part[:, LANES:]
                columns.append(
                    jnp.concatenate([real * cos + imag * sin, imag * cos - real * sin], axis=0)
                )
            rights[pair] = right_operand(jnp.concatenate(columns, axis=1))
        for pair in pairs:
            spread = dot(scatter_ref[...], rights[pair])
            for index in range(2):
                part = spread[:, index * LANES : (index + 1) * LANES]
                first, second = to_modes(part[:group_size], part[group_size:])
                picked = pl.ds(2 * pair + index, group_size, stride=rows)
                out_back[0, picked, :] = first
                out_back[1, picked, :] = second
        for side in range(2):
            exchange(out_back.at[side], in_back.at[side], back_send.at[side], back_recv.at[side])

    top_rows = lax.broadcasted_iota(jnp.int32, (8, degrees), 0) < 4

    def precondition(side, field):
        high = field.astype(jnp.bfloat16).astype(jnp.float32)
        terms = [part.reshape(LANES // 8, 8, degrees) for part in (high, field - high)]
        terms = jnp.stack(terms, axis=1).reshape(2 * LANES, degrees).astype(jnp.bfloat16)
        for pair in range(half // 2):
            left = terms[16 * pair : 16 * pair + 16]
            left = jnp.concatenate([left, left], axis=1)
            found = []
            for index in range(2):
                base = (side * half + 2 * pair + index) * 2 * degrees
                where = pl.ds(pl.multiple_of(base, 2 * degrees), 2 * degrees)
                both = dot(left, tau_terms[where, :])
                found.append(both[:8] + both[8:])
            applied[side, pair] = jnp.where(top_rows, found[0], found[1])

    stat_row = lax.broadcasted_iota(jnp.int32, (8, LANES), 0)
    packed = stat_row == lax.broadcasted_iota(jnp.int32, (8, LANES), 1)

    def send_stats():
        sums = []
        for chosen in (low_rows, ~low_rows):
            for known in range(KRYLOV + 1):
                sums.append(
                    jnp.sum(jnp.where(chosen, partial[known], 0.0), axis=0, keepdims=True)
                )
        sums = jnp.sum(jnp.concatenate(sums, axis=0), axis=1, keepdims=True)
        out_stat[...] = jnp.sum(jnp.where(packed, sums, 0.0), axis=0, keepdims=True)
        for peer, place in peers():
            pltpu.make_async_remote_copy(
                src_ref=out_stat,
                dst_ref=in_stat.at[me],
                send_sem=stat_send,
                recv_sem=stat_recv,
                device_id=place,
                device_id_type=pl.DeviceIdType.MESH,
            ).start()
        pltpu.make_async_copy(out_stat, in_stat.at[me], stat_recv).start()

    def receive_stats():
        sent = pl.ds(0, group_size - 1)
        pltpu.make_async_copy(in_stat.at[sent], in_stat.at[sent], stat_send).wait()
        pltpu.make_async_copy(in_stat, in_stat, stat_recv).wait()
        total = jnp.sum(in_stat[...], axis=0)
        return jnp.sum(jnp.where(packed, total, 0.0), axis=1, keepdims=True)

    def by_flow(stats, known):
        low = jnp.broadcast_to(stats[known : known + 1], (8, LANES))
        high = jnp.broadcast_to(stats[known + KRYLOV + 1 : known + KRYLOV + 2], (8, LANES))
        return jnp.concatenate(
            [jnp.where(low_flow, low, high), jnp.where(low_rows, low, high)], axis=0
        )

    def for_points(value):
        return value[:1]

    def for_coefs(value):
        return jnp.concatenate([value[8:], value[8:]], axis=1)[None]

    chunks, chunk = stage.shape[:2]

    def fetch(index):
        where = pl.ds(pl.multiple_of(index * chunk, chunk), chunk)
        return pltpu.make_async_copy(taus_ref.at[where, :], stage.at[index], stage_sem.at[index])

    def fetch_step(index, carry):
        fetch(index).start()
        return carry

    lax.fori_loop(0, chunks, fetch_step, 0)

    def spread_rows(field_ref):
        for flow in range(2):
            for part in range(2):
                for side in range(2):
                    rows_of_part = field_ref[flow, part, pl.ds(side * half, half), :]
                    where = pl.ds(2 * flow + part, half, stride=4)
                    for column in range(2):
                        lanes = slice(column * LANES, (column + 1) * LANES)
                        ordered[side, column, where, :] = rows_of_part[:, lanes]

    def in_order(side):
        return jnp.concatenate([ordered[side, 0], ordered[side, 1]], axis=1)

    spread_rows(forcing_ref)
    vectors[...] = jnp.zeros_like(vectors)
    images[...] = jnp.zeros_like(images)
    for side in range(2):
        driven[side] = rows_of(in_order(side))
    spread_rows(start_ref)
    for side in range(2):
        vectors[0, side] = in_order(side).reshape(LANES // 8, 8, degrees)
    for side in range(2):
        send_values(side, vectors[0, side])

    def load(index, carry):
        fetch(index).wait()
        for mode in range(chunk // degrees):
            operand = row_operand(stage[index, mode * degrees : (mode + 1) * degrees])
            high, low = split(dot_rows(to_degrees_ref[...], operand))
            base = (index * (chunk // degrees) + mode) * 2 * degrees
            base = pl.multiple_of(base, 2 * degrees)
            tau_terms[pl.ds(base, degrees), :] = high
            tau_terms[pl.ds(base + degrees, degrees), :] = low
        return carry

    lax.fori_loop(0, chunks // 2, load, 0)

    receive_points()
    for pair in pairs:
        points = points_of_rows(pair)
        for part in range(2):
            images[0, part, pair_rows(pair), :] = points[part]
        keep_product(pair, STRENGTH * points[0] * points[1])
    send_products()
    steps = NEWTON * (KRYLOV + 1)

    def iteration(index, carry):
        phase = lax.rem(index, KRYLOV + 1)
        opening = phase == 0

        @pl.when(index == 0)
        def _():
            lax.fori_loop(chunks // 2, chunks, load, 0)

        drive = jnp.where(opening, 1.0, 0.0)
        partial[...] = jnp.zeros_like(partial)

        def half_step(side, carry):
            finish_exchange(
                out_back.at[side], in_back.at[side], back_send.at[side], back_recv.at[side]
            )
            precondition(side, (in_back[side] - drive * driven[side]).T)
            whole = vectors[phase, side] + applied[side]
            applied[side] = whole

            def add_stat(known, other):
                summed = jnp.sum(other * whole, axis=0)
                partial[known] += summed[:, :LANES] + summed[:, LANES:]

            for known in range(KRYLOV):
                add_stat(known, vectors[known + 1, side])
            add_stat(KRYLOV, whole)

            @pl.when(side == 1)
            def _():
                send_stats()

            @pl.when(phase < KRYLOV)
            def _():
                send_values(side, applied[side])

            return carry

        lax.fori_loop(0, 2, half_step, 0)
        stats = receive_stats()
        inner_products = [
            jnp.where(known < phase, by_flow(stats, known), 0.0) for known in range(KRYLOV)
        ]
        square = by_flow(stats, KRYLOV)
        for value in inner_products:
            square = square - value * value
        length = jnp.sqrt(square)
        scale = jnp.where(opening, -1.0, 1.0) / length
        for known in range(KRYLOV):
            history[phase, known] = inner_products[known]
        history[phase, KRYLOV] = length

        @pl.when(phase < KRYLOV)
        def _():
            for side in range(2):
                whole = applied[side]
                for known in range(KRYLOV):
                    whole = whole - for_coefs(inner_products[known]) * vectors[known + 1, side]
                vectors[phase + 1, side] = for_coefs(scale) * whole
            receive_points()
            for pair in pairs:
                where = pair_rows(pair)
                fresh = []
                for part, whole in enumerate(points_of_rows(pair)):
                    for known in range(KRYLOV):
                        factor = for_points(inner_products[known])
                        whole = whole - factor * images[known + 1, part, where, :]
                    fresh.append(for_points(scale) * whole)
                    images[phase + 1, part, where, :] = fresh[part]
                crossed = images[0, 0, where, :] * fresh[1] + fresh[0] * images[0, 1, where, :]
                keep_product(pair, STRENGTH * crossed)
            send_products()

        @pl.when(phase == KRYLOV)
        def _():
            matrix = []
            for column in range(KRYLOV):
                entries = [history[column + 1, known] for known in range(column + 1)]
                matrix.append(entries + [history[column + 1, KRYLOV]])
            solved = least_squares(matrix, history[0, KRYLOV])
            for side in range(2):
                whole = vectors[0, side]
                for known in range(KRYLOV):
                    whole = whole + for_coefs(solved[known]) * vectors[known + 1, side]
                vectors[0, side] = whole

            @pl.when(index + 1 < steps)
            def _():
                for pair in pairs:
                    where = pair_rows(pair)
                    fresh = []
                    for part in range(2):
                        whole = images[0, part, where, :]
                        for known in range(KRYLOV):
                            factor = for_points(solved[known])
                            whole = whole + factor * images[known + 1, part, where, :]
                        fresh.append(whole)
                        images[0, part, where, :] = whole
                    keep_product(pair, STRENGTH * fresh[0] * fresh[1])
                send_products()

        return carry

    lax.fori_loop(0, steps, iteration, 0)
    for side in range(2):
        whole = vectors[0, side].reshape(LANES, degrees)
        ordered[side, 0] = whole[:, :LANES]
        ordered[side, 1] = whole[:, LANES:]
    for flow in range(2):
        for part in range(2):
            for side in range(2):
                where = pl.ds(2 * flow + part, half, stride=4)
                out_ref[flow, part, pl.ds(side * half, half), :] = jnp.concatenate(
                    [ordered[side, 0, where, :], ordered[side, 1, where, :]], axis=1
                )


def solve_flows(start, forcing, taus):
    group_size = lax.axis_size(AXES)
    minor = lax.axis_size(AXES[1])
    batch, parts, local_modes, degrees = start.shape
    rows = degrees // group_size
    inner = 2 * group_size
    half = local_modes // 2
    tables = tables_of(local_modes, group_size, degrees)
    sizes = (group_size, minor, local_modes, rows, degrees, inner)

    coefs = (2, LANES // 8, 8, degrees)

    field = (2, degrees, LANES)
    image = (2, rows * inner, LANES)
    chunk = 4 * degrees
    chunks = local_modes // 4
    vmem = pl.BlockSpec(memory_space=pltpu.VMEM)
    out = pl.pallas_call(
        functools.partial(flow_solver, sizes),
        out_shape=jax.ShapeDtypeStruct(start.shape, jnp.float32),
        in_specs=[vmem, vmem, pl.BlockSpec(memory_space=pl.ANY)] + [vmem] * len(tables),
        out_specs=vmem,
        scratch_shapes=[
            pltpu.VMEM((local_modes * 2 * degrees, degrees), jnp.bfloat16),
            pltpu.VMEM((chunks, chunk, degrees), jnp.float32),
            pltpu.VMEM((KRYLOV + 1,) + coefs, jnp.float32),
            pltpu.VMEM(coefs, jnp.float32),
            pltpu.VMEM((KRYLOV + 1, 8, LANES), jnp.float32),
            pltpu.VMEM(field, jnp.float32),
            pltpu.VMEM((KRYLOV + 1,) + image, jnp.float32),
            pltpu.VMEM((2, 2, LANES, LANES), jnp.float32),
            pltpu.VMEM((rows // 2, 4 * inner, 2 * LANES), jnp.float32),
            pltpu.VMEM((rows // 2, 4 * inner, 4 * LANES), jnp.bfloat16),
            pltpu.VMEM((rows // 2, 2 * inner, 3 * LANES), jnp.bfloat16),
            pltpu.VMEM((rows // 2, 6 * inner, 2 * LANES), jnp.bfloat16),
            pltpu.VMEM(field, jnp.float32),
            pltpu.VMEM(field, jnp.float32),
            pltpu.VMEM(field, jnp.float32),
            pltpu.VMEM(field, jnp.float32),
            pltpu.VMEM((1, LANES), jnp.float32),
            pltpu.VMEM((group_size, 1, LANES), jnp.float32),
            pltpu.VMEM((KRYLOV + 1, KRYLOV + 1, 16, LANES), jnp.float32),
            pltpu.SemaphoreType.DMA((chunks,)),
        ]
        + [pltpu.SemaphoreType.DMA((2,))] * 4
        + [pltpu.SemaphoreType.DMA] * 2,
        compiler_params=pltpu.CompilerParams(
            has_side_effects=True, vmem_limit_bytes=56 * 1024 * 1024
        ),
    )(
        start,
        forcing,
        taus.reshape(local_modes * degrees, degrees),
        *[jnp.asarray(table) for table in tables],
    )
    return out


def fits_kernel(start):
    batch, parts, local_modes, degrees = start.shape
    group = lax.axis_size(AXES)
    rows = degrees // group
    fits = (batch, parts, rows, batch * local_modes) == (2, 2, 8, LANES)
    return fits and group & (group - 1) == 0


def local_step(start, forcing, taus):
    if fits_kernel(start):
        return solve_flows(start, forcing, taus)
    return shards(start, forcing, taus)


def solution(mesh):
    return jax.shard_map(
        local_step,
        mesh=mesh,
        in_specs=(
            P(None, None, ("modes", "cheb"), None),
            P(None, None, ("modes", "cheb"), None),
            P(("modes", "cheb"), None, None),
        ),
        out_specs=P(None, None, ("modes", "cheb"), None),
        check_vma=False,
    )
```

```python
import functools
import math

import jax
import jax.numpy as jnp
import numpy as np
from jax import lax
from jax.experimental import pallas as pl
from jax.experimental.pallas import tpu as pltpu
from jax.sharding import PartitionSpec as P

NEWTON = 2
KRYLOV = 3


PREC = lax.Precision.HIGH
STRENGTH = 0.1
AXES = ("modes", "cheb")
STAT_LANES = 128
LANES = 128


def cheb_rows(degree_count):
    degree = jnp.arange(degree_count, dtype=jnp.int32)[:, None]
    node = 2 * jnp.arange(degree_count, dtype=jnp.int32)[None, :] + 1
    turns = degree * node % (4 * degree_count)
    return jnp.cos(2.0 * math.pi / (4 * degree_count) * turns.astype(jnp.float32))


def phase_table(row_count, col_count, period):
    row_index = jnp.arange(row_count, dtype=jnp.int32)[:, None]
    col_index = jnp.arange(col_count, dtype=jnp.int32)[None, :]
    turns = row_index * col_index % period
    angle = 2.0 * math.pi / period * turns.astype(jnp.float32)
    return (jnp.cos(angle), jnp.sin(angle))


def least_squares(matrix, beta_norm):
    steps_count = len(matrix)
    target = [beta_norm] + [jnp.zeros_like(beta_norm) for row_index in range(steps_count)]
    cosines = []
    sines_list = []
    for col_index in range(steps_count):
        column = matrix[col_index]
        for row_index in range(col_index):
            upper_entry = (
                cosines[row_index] * column[row_index]
                + sines_list[row_index] * column[row_index + 1]
            )
            lower_entry = (
                cosines[row_index] * column[row_index + 1]
                - sines_list[row_index] * column[row_index]
            )
            column[row_index] = upper_entry
            column[row_index + 1] = lower_entry
        radius = jnp.sqrt(
            column[col_index] * column[col_index] + column[col_index + 1] * column[col_index + 1]
        )
        cosines.append(column[col_index] / radius)
        sines_list.append(column[col_index + 1] / radius)
        column[col_index] = radius
        target[col_index + 1] = -sines_list[col_index] * target[col_index]
        target[col_index] = cosines[col_index] * target[col_index]
    solved = [None] * steps_count
    for row_index in reversed(range(steps_count)):
        partial_sum = target[row_index]
        for col_index in range(row_index + 1, steps_count):
            partial_sum = partial_sum - matrix[col_index][row_index] * solved[col_index]
        solved[row_index] = partial_sum / matrix[row_index][row_index]
    return solved


def shards(start, forcing, taus):
    group_size = lax.axis_size(AXES)
    batch, parts, local_modes, degrees = start.shape
    total_modes = local_modes * group_size
    points_count = 2 * total_modes
    outer_len = max(2 ** ((points_count.bit_length() - 1) // 2), local_modes)
    inner_len = points_count // outer_len
    half_inner = inner_len // 2
    split = outer_len // local_modes
    rows = degrees // group_size
    block_lanes = batch * 2 * local_modes
    fields = rows * batch
    spread = 1.0 / math.sqrt(total_modes * degrees)
    gather_factor = math.sqrt(total_modes * degrees) / points_count
    cheb_table = cheb_rows(degrees)
    tau_keep = (jnp.arange(degrees) < degrees - 2).astype(jnp.float32)
    coef_weights = jnp.where(jnp.arange(degrees) == 0, 1.0, 2.0).astype(jnp.float32) / degrees
    back_table = cheb_table * (coef_weights * tau_keep)[:, None]

    section_cos, section_sin = phase_table(inner_len, half_inner, inner_len)
    value_table = jnp.stack([section_cos, section_sin])
    slope_table = jnp.stack([-section_sin, section_cos])
    back_cos, back_sin = section_cos.T, section_sin.T
    twist_cos, twist_sin = phase_table(inner_len, outer_len, points_count)
    final_cos, final_sin = phase_table(outer_len, outer_len, outer_len)
    turn_cos = (
        twist_cos[:, :, None] * final_cos[None] - twist_sin[:, :, None] * final_sin[None]
    )
    turn_sin = (
        twist_sin[:, :, None] * final_cos[None] + twist_cos[:, :, None] * final_sin[None]
    )
    turn_table = lax.optimization_barrier(
        jnp.concatenate([turn_cos, -turn_sin, -turn_sin, -turn_cos], axis=1)
    )
    mode = (
        outer_len * jnp.arange(half_inner, dtype=jnp.int32)[:, None]
        + jnp.arange(outer_len, dtype=jnp.int32)[None, :]
    )
    paired_mode = jnp.concatenate([mode, mode], axis=1)[:, None, :]
    weights = jnp.where(paired_mode == 0, 1.0, 2.0).astype(jnp.float32) * spread
    slope_weights = weights * (16.0 * paired_mode.astype(jnp.float32) / total_modes)

    def exchange(blocks):
        return lax.all_to_all(blocks, AXES, split_axis=0, concat_axis=0, tiled=True)

    def stat_block(stats):
        flat = jnp.pad(stats.reshape(-1), (0, STAT_LANES - stats.size))
        return jnp.broadcast_to(flat, (group_size, rows, STAT_LANES))

    def read_stats(received, shape):
        flat = jnp.sum(received[:, 0, :], axis=0)
        return flat[: math.prod(shape)].reshape(shape)

    def to_points(coefs, stats):
        values = jnp.einsum("ni,brkn->ibrk", cheb_table, coefs, precision=PREC)
        blocks = values.reshape(group_size, rows, block_lanes)
        if stats is not None:
            blocks = jnp.concatenate([blocks, stat_block(stats)], axis=2)
        received = exchange(blocks)
        summed = None
        if stats is not None:
            summed = read_stats(received[:, :, block_lanes:], stats.shape)
            received = received[:, :, :block_lanes]
        spectrum = received.reshape(half_inner, split, rows, batch, 2, local_modes)
        spectrum = spectrum.transpose(0, 2, 3, 4, 1, 5).reshape(
            half_inner, fields, 2 * outer_len
        )

        def points_of(table, weighted):
            turned = jnp.einsum("sjq,qyl->jysl", table, weighted, precision=PREC)
            turned = turned.reshape(inner_len, fields, 4 * outer_len)
            return jnp.einsum("jyl,jlt->jyt", turned, turn_table, precision=PREC)

        values = points_of(value_table, spectrum * weights)
        slopes = points_of(slope_table, spectrum * slope_weights)
        return (values, slopes), summed

    def to_coefficients(points):
        turned = jnp.einsum("jyt,jlt->jyl", points, turn_table, precision=PREC) * gather_factor
        direct = turned[:, :, : 2 * outer_len].reshape(inner_len, -1)
        swapped = turned[:, :, 2 * outer_len :].reshape(inner_len, -1)
        spectrum = jnp.dot(back_cos, direct, precision=PREC) + jnp.dot(
            back_sin, swapped, precision=PREC
        )
        blocks = spectrum.reshape(half_inner, rows, batch, 2, split, local_modes)
        blocks = blocks.transpose(0, 4, 1, 2, 3, 5).reshape(group_size, rows, block_lanes)
        received = exchange(blocks).reshape(degrees, batch, 2, local_modes)
        return jnp.einsum("ibrk,ni->brkn", received, back_table, precision=PREC)

    def precondition(coefs):
        return jnp.einsum("kam,brkm->brka", taus, coefs, precision=PREC)

    def on_points(scale):
        return jnp.tile(scale, rows)[None, :, None]

    def on_coefs(scale):
        return scale[:, None, None, None]

    iterate = start
    kept_forcing = forcing * tau_keep
    base, nothing = to_points(iterate, None)
    for newton_step in range(NEWTON):
        base_points, base_slopes = base
        residual = iterate + precondition(
            to_coefficients(STRENGTH * base_points * base_slopes) - kept_forcing
        )
        local_square = jnp.sum(residual * residual, axis=(1, 2, 3))
        image, squared = to_points(residual, local_square)
        beta_norm = jnp.sqrt(squared)
        krylov_basis = [-residual / on_coefs(beta_norm)]
        images = [tuple(-part / on_points(beta_norm) for part in image)]
        hessen = []
        for column in range(KRYLOV):
            probe_points, probe_slopes = images[column]
            product = STRENGTH * (base_points * probe_slopes + probe_points * base_slopes)
            applied = krylov_basis[column] + precondition(to_coefficients(product))
            local_stats = jnp.stack(
                [jnp.sum(vector * applied, axis=(1, 2, 3)) for vector in krylov_basis + [applied]],
                axis=1,
            )
            last = column == KRYLOV - 1
            if last:
                stats = read_stats(exchange(stat_block(local_stats)), local_stats.shape)
            else:
                image, stats = to_points(applied, local_stats)
            projections, square = stats[:, :-1], stats[:, -1]
            length = jnp.sqrt(square - jnp.sum(projections * projections, axis=1))
            hessen.append(jnp.concatenate([projections, length[:, None]], axis=1))
            if not last:
                for index in range(column + 1):
                    applied = applied - on_coefs(projections[:, index]) * krylov_basis[index]
                    image = tuple(
                        part - on_points(projections[:, index]) * known
                        for part, known in zip(image, images[index])
                    )
                krylov_basis.append(applied / on_coefs(length))
                images.append(tuple(part / on_points(length) for part in image))
        matrix = [
            [hessen[column][:, row] for row in range(column + 2)] for column in range(KRYLOV)
        ]
        solved = least_squares(matrix, beta_norm)
        for column in range(KRYLOV):
            iterate = iterate + on_coefs(solved[column]) * krylov_basis[column]
            base = tuple(
                part + on_points(solved[column]) * known
                for part, known in zip(base, images[column])
            )
    return iterate


def split_table(table):
    table = np.asarray(table, np.float32)
    high = table.astype(jnp.bfloat16)
    low = (table - high.astype(np.float32)).astype(jnp.bfloat16)
    return high, low


def left_table(table):
    high, low = split_table(table)
    return np.concatenate([high, low, high], axis=1)


def tables_of(local_modes, group_size, degrees):
    total = local_modes * group_size
    points = 2 * total
    inner = points // local_modes
    half = local_modes // 2
    spread = 1.0 / math.sqrt(total * degrees)
    degree = np.arange(degrees)[:, None]
    node = 2 * np.arange(degrees)[None, :] + 1
    cheb = np.cos(2.0 * np.pi / (4 * degrees) * (degree * node % (4 * degrees)))
    coef_weights = np.where(np.arange(degrees) == 0, 1.0, 2.0) / degrees
    keep = np.arange(degrees) < degrees - 2
    to_rows = left_table(cheb.T)
    to_degrees = left_table((cheb * (coef_weights * keep)[:, None]).T)

    j_low = np.arange(inner)[:, None]
    source = np.arange(group_size)[None, :]
    angle = 2.0 * np.pi / inner * (j_low * source % inner)
    cos, sin = np.cos(angle), np.sin(angle)
    real = np.concatenate([cos, -sin], axis=1)
    imag = np.concatenate([sin, cos], axis=1)
    wave = np.tile(16.0 * local_modes * source / total, (1, 2))
    gather = 2.0 * spread * np.concatenate([real, imag, real * wave, imag * wave], axis=0)
    gather = left_table(gather)
    scatter = np.concatenate(
        [np.concatenate([cos.T, sin.T], axis=1), np.concatenate([-sin.T, cos.T], axis=1)], axis=0
    )
    scatter = left_table(scatter * math.sqrt(total * degrees) / points)

    lane = np.arange(2 * local_modes)
    lane_mode = (lane // 4 + half * (lane % 2))[None, :]
    lane_flow = lane // 2 % 2
    twist = 2.0 * np.pi / points * (j_low * lane_mode)
    wave_low = np.broadcast_to(16.0 * lane_mode / total, twist.shape)
    twist = np.stack([np.cos(twist), np.sin(twist), wave_low]).astype(np.float32)

    final = lane_mode.T * np.tile(np.arange(local_modes), 2)[None, :] % local_modes
    final = 2.0 * np.pi / local_modes * final
    same = lane_flow[:, None] == lane[None, :] // local_modes
    cos_high, cos_low = split_table(same * np.cos(final))
    sin_high, sin_low = split_table(same * np.sin(final))
    cos_row = np.concatenate([cos_high, cos_low], axis=1)
    sin_row = np.concatenate([-sin_high, -sin_low], axis=1)
    finish = np.concatenate([cos_row, sin_row, cos_row, sin_row], axis=0)
    high_row = np.concatenate([cos_high.T, -sin_high.T], axis=1)
    low_row = np.concatenate([cos_low.T, -sin_low.T], axis=1)
    begin = np.concatenate([high_row, high_row, low_row], axis=0)
    return to_rows, to_degrees, gather, scatter, twist, finish, begin


def split(value):
    high = value.astype(jnp.bfloat16)
    return high, (value - high.astype(jnp.float32)).astype(jnp.bfloat16)


def right_operand(value):
    high, low = split(value)
    return jnp.concatenate([high, high, low], axis=0)


def dot(left, right):
    return jnp.dot(left, right, preferred_element_type=jnp.float32)


def dot_rows(left, right):
    dims = (((1,), (1,)), ((), ()))
    return lax.dot_general(left, right, dims, preferred_element_type=jnp.float32)


def row_operand(value):
    high, low = split(value)
    return jnp.concatenate([high, high, low], axis=1)


def flow_solver(
    sizes,
    start_ref,
    forcing_ref,
    taus_ref,
    to_rows_hbm,
    to_degrees_hbm,
    gather_hbm,
    scatter_hbm,
    twist_hbm,
    finish_hbm,
    begin_hbm,
    out_ref,
    to_rows_ref,
    to_degrees_ref,
    gather_ref,
    scatter_ref,
    twist_ref,
    finish_ref,
    begin_ref,
    tau_terms,
    stage,
    vectors,
    applied,
    partial,
    driven,
    images,
    ordered,
    summed,
    lefts,
    products,
    rights,
    out_fwd,
    in_fwd,
    out_back,
    in_back,
    out_stat,
    in_stat,
    history,
    stage_sem,
    table_sem,
    fwd_send,
    fwd_recv,
    back_send,
    back_recv,
    stat_send,
    stat_recv,
):
    group_size, minor, local_modes, rows, degrees, inner = sizes
    half = local_modes // 2
    me = lax.axis_index(AXES[0]) * minor + lax.axis_index(AXES[1])
    lane = lax.broadcasted_iota(jnp.int32, (1, LANES), 1)
    even_lane = lane % 2 == 0
    low_flow = lane < local_modes
    low_rows = lax.broadcasted_iota(jnp.int32, (8, LANES), 0) % 4 < 2

    def own_rows(index):
        return pl.ds(pl.multiple_of(index * rows, rows), rows)

    flips = []
    for bit in range(group_size.bit_length() - 1):
        flips.append((1 << bit) - (2 << bit) * lax.rem(me // (1 << bit), 2))

    def peers():
        for distance in reversed(range(1, group_size)):
            peer = me
            for bit, flip in enumerate(flips):
                if distance >> bit & 1:
                    peer = peer + flip
            yield peer, (peer // minor, lax.rem(peer, minor))

    def exchange(src, dst, send_sem, recv_sem):
        for peer, place in peers():
            pltpu.make_async_remote_copy(
                src_ref=src.at[own_rows(peer), :],
                dst_ref=dst.at[own_rows(me), :],
                send_sem=send_sem,
                recv_sem=recv_sem,
                device_id=place,
                device_id_type=pl.DeviceIdType.MESH,
            ).start()
        pltpu.make_async_copy(
            src.at[own_rows(me), :], dst.at[own_rows(me), :], recv_sem
        ).start()

    def finish_exchange(src, dst, send_sem, recv_sem):
        sent = pl.ds(0, (group_size - 1) * rows)
        pltpu.make_async_copy(src.at[sent, :], dst.at[sent, :], send_sem).wait()
        pltpu.make_async_copy(src, dst, recv_sem).wait()

    def to_modes(first, second):
        turned = pltpu.roll(second, 1, 1)
        back = pltpu.roll(first, LANES - 1, 1)
        return jnp.where(even_lane, first, turned), jnp.where(even_lane, back, second)

    def rows_of(field):
        return dot_rows(to_rows_ref[...], row_operand(field.reshape(LANES, degrees)))

    def send_values(side, field):
        constant = jnp.logical_and(me + side == 0, lane < 4)
        out_fwd[side] = rows_of(field) * jnp.where(constant, 0.5, 1.0)
        exchange(out_fwd.at[side], in_fwd.at[side], fwd_send.at[side], fwd_recv.at[side])

    pairs = range(rows // 2)

    def sums_over_sources():
        for pair in pairs:
            columns = []
            for row in (2 * pair, 2 * pair + 1):
                picked = pl.ds(row, group_size, stride=rows)
                real, imag = to_modes(in_fwd[0, picked, :], in_fwd[1, picked, :])
                columns.append(jnp.concatenate([real, imag], axis=0))
            operand = right_operand(jnp.concatenate(columns, axis=1))
            summed[pair] = dot(gather_ref[...], operand)
        cos, sin, low = twist_ref[0], twist_ref[1], twist_ref[2]
        for row in range(rows):
            pair, index = divmod(row, 2)
            lanes = slice(index * LANES, (index + 1) * LANES)
            real, imag, wave_real, wave_imag = (
                summed[pair, n * inner : (n + 1) * inner, lanes] for n in range(4)
            )
            slope_real = -(wave_imag + low * imag)
            slope_imag = wave_real + low * real
            for part, (re, im) in enumerate(((real, imag), (slope_real, slope_imag))):
                re_high, re_low = split(re * cos - im * sin)
                im_high, im_low = split(re * sin + im * cos)
                where = slice((2 * part + index) * inner, (2 * part + index + 1) * inner)
                lefts[pair, where] = jnp.concatenate([re_high, im_high, re_low, im_low], axis=1)

    def points_of_rows(pair):
        wide = dot(lefts[pair], finish_ref[...])
        points = wide[:, :LANES] + wide[:, LANES:]
        return points[: 2 * inner], points[2 * inner :]

    def receive_points():
        for side in range(2):
            finish_exchange(
                out_fwd.at[side], in_fwd.at[side], fwd_send.at[side], fwd_recv.at[side]
            )
        sums_over_sources()

    def pair_rows(pair):
        return pl.ds(2 * pair * inner, 2 * inner)

    def keep_product(pair, product):
        high, low = split(product)
        products[pair] = jnp.concatenate([high, low, high], axis=1)

    def send_products():
        cos, sin = twist_ref[0], twist_ref[1]
        for pair in pairs:
            turned = dot(products[pair], begin_ref[...])
            columns = []
            for index in range(2):
                part = turned[index * inner : (index + 1) * inner]
                real, imag = part[:, :LANES], part[:, LANES:]
                columns.append(
                    jnp.concatenate([real * cos + imag * sin, imag * cos - real * sin], axis=0)
                )
            rights[pair] = right_operand(jnp.concatenate(columns, axis=1))
        for pair in pairs:
            spread = dot(scatter_ref[...], rights[pair])
            for index in range(2):
                part = spread[:, index * LANES : (index + 1) * LANES]
                first, second = to_modes(part[:group_size], part[group_size:])
                picked = pl.ds(2 * pair + index, group_size, stride=rows)
                out_back[0, picked, :] = first
                out_back[1, picked, :] = second
        for side in range(2):
            exchange(out_back.at[side], in_back.at[side], back_send.at[side], back_recv.at[side])

    top_rows = lax.broadcasted_iota(jnp.int32, (8, degrees), 0) < 4

    def precondition(side, field):
        high = field.astype(jnp.bfloat16).astype(jnp.float32)
        terms = [part.reshape(LANES // 8, 8, degrees) for part in (high, field - high)]
        terms = jnp.stack(terms, axis=1).reshape(2 * LANES, degrees).astype(jnp.bfloat16)
        for pair in range(half // 2):
            left = terms[16 * pair : 16 * pair + 16]
            left = jnp.concatenate([left, left], axis=1)
            found = []
            for index in range(2):
                base = (side * half + 2 * pair + index) * 2 * degrees
                where = pl.ds(pl.multiple_of(base, 2 * degrees), 2 * degrees)
                both = dot(left, tau_terms[where, :])
                found.append(both[:8] + both[8:])
            applied[side, pair] = jnp.where(top_rows, found[0], found[1])

    stat_row = lax.broadcasted_iota(jnp.int32, (8, LANES), 0)
    packed = stat_row == lax.broadcasted_iota(jnp.int32, (8, LANES), 1)

    def send_stats():
        sums = []
        for chosen in (low_rows, ~low_rows):
            for known in range(KRYLOV + 1):
                sums.append(
                    jnp.sum(jnp.where(chosen, partial[known], 0.0), axis=0, keepdims=True)
                )
        sums = jnp.sum(jnp.concatenate(sums, axis=0), axis=1, keepdims=True)
        out_stat[...] = jnp.sum(jnp.where(packed, sums, 0.0), axis=0, keepdims=True)
        for peer, place in peers():
            pltpu.make_async_remote_copy(
                src_ref=out_stat,
                dst_ref=in_stat.at[me],
                send_sem=stat_send,
                recv_sem=stat_recv,
                device_id=place,
                device_id_type=pl.DeviceIdType.MESH,
            ).start()
        pltpu.make_async_copy(out_stat, in_stat.at[me], stat_recv).start()

    def receive_stats():
        sent = pl.ds(0, group_size - 1)
        pltpu.make_async_copy(in_stat.at[sent], in_stat.at[sent], stat_send).wait()
        pltpu.make_async_copy(in_stat, in_stat, stat_recv).wait()
        total = jnp.sum(in_stat[...], axis=0)
        return jnp.sum(jnp.where(packed, total, 0.0), axis=1, keepdims=True)

    def by_flow(stats, known):
        low = jnp.broadcast_to(stats[known : known + 1], (8, LANES))
        high = jnp.broadcast_to(stats[known + KRYLOV + 1 : known + KRYLOV + 2], (8, LANES))
        return jnp.concatenate(
            [jnp.where(low_flow, low, high), jnp.where(low_rows, low, high)], axis=0
        )

    def for_points(value):
        return value[:1]

    def for_coefs(value):
        return jnp.concatenate([value[8:], value[8:]], axis=1)[None]

    chunks, chunk = stage.shape[:2]

    def fetch(index):
        where = pl.ds(pl.multiple_of(index * chunk, chunk), chunk)
        return pltpu.make_async_copy(taus_ref.at[where, :], stage.at[index], stage_sem.at[index])

    def fetch_step(index, carry):
        fetch(index).start()
        return carry

    barrier = pltpu.get_barrier_semaphore()
    for _, place in peers():
        pl.semaphore_signal(
            barrier, inc=1, device_id=place, device_id_type=pl.DeviceIdType.MESH
        )
    tables = (
        (to_rows_hbm, to_rows_ref),
        (to_degrees_hbm, to_degrees_ref),
        (gather_hbm, gather_ref),
        (scatter_hbm, scatter_ref),
        (twist_hbm, twist_ref),
        (finish_hbm, finish_ref),
        (begin_hbm, begin_ref),
    )
    tables = [
        pltpu.make_async_copy(src, dst, table_sem.at[index])
        for index, (src, dst) in enumerate(tables)
    ]
    for copy in tables:
        copy.start()
    lax.fori_loop(0, chunks, fetch_step, 0)

    def spread_rows(field_ref):
        for flow in range(2):
            for part in range(2):
                for side in range(2):
                    rows_of_part = field_ref[flow, part, pl.ds(side * half, half), :]
                    where = pl.ds(2 * flow + part, half, stride=4)
                    for column in range(2):
                        lanes = slice(column * LANES, (column + 1) * LANES)
                        ordered[side, column, where, :] = rows_of_part[:, lanes]

    def in_order(side):
        return jnp.concatenate([ordered[side, 0], ordered[side, 1]], axis=1)

    vectors[...] = jnp.zeros_like(vectors)
    images[...] = jnp.zeros_like(images)
    spread_rows(start_ref)
    for copy in tables:
        copy.wait()
    pl.semaphore_wait(barrier, group_size - 1)
    for side in range(2):
        vectors[0, side] = in_order(side).reshape(LANES // 8, 8, degrees)
    for side in range(2):
        send_values(side, vectors[0, side])
    spread_rows(forcing_ref)
    for side in range(2):
        driven[side] = rows_of(in_order(side))

    def load(index, carry):
        fetch(index).wait()
        for mode in range(chunk // degrees):
            operand = row_operand(stage[index, mode * degrees : (mode + 1) * degrees])
            high, low = split(dot_rows(to_degrees_ref[...], operand))
            base = (index * (chunk // degrees) + mode) * 2 * degrees
            base = pl.multiple_of(base, 2 * degrees)
            tau_terms[pl.ds(base, degrees), :] = high
            tau_terms[pl.ds(base + degrees, degrees), :] = low
        return carry

    lax.fori_loop(0, chunks // 2, load, 0)

    receive_points()
    for pair in pairs:
        points = points_of_rows(pair)
        for part in range(2):
            images[0, part, pair_rows(pair), :] = points[part]
        keep_product(pair, STRENGTH * points[0] * points[1])
    send_products()
    steps = NEWTON * (KRYLOV + 1)

    def iteration(index, carry):
        phase = lax.rem(index, KRYLOV + 1)
        opening = phase == 0

        @pl.when(index == 0)
        def _():
            lax.fori_loop(chunks // 2, chunks, load, 0)

        drive = jnp.where(opening, 1.0, 0.0)
        partial[...] = jnp.zeros_like(partial)

        def half_step(side, carry):
            finish_exchange(
                out_back.at[side], in_back.at[side], back_send.at[side], back_recv.at[side]
            )
            precondition(side, (in_back[side] - drive * driven[side]).T)
            whole = vectors[phase, side] + applied[side]
            applied[side] = whole

            def add_stat(known, other):
                summed = jnp.sum(other * whole, axis=0)
                partial[known] += summed[:, :LANES] + summed[:, LANES:]

            for known in range(KRYLOV):
                add_stat(known, vectors[known + 1, side])
            add_stat(KRYLOV, whole)

            @pl.when(side == 1)
            def _():
                send_stats()

            @pl.when(phase < KRYLOV)
            def _():
                send_values(side, applied[side])

            return carry

        lax.fori_loop(0, 2, half_step, 0)
        stats = receive_stats()
        inner_products = [
            jnp.where(known < phase, by_flow(stats, known), 0.0) for known in range(KRYLOV)
        ]
        square = by_flow(stats, KRYLOV)
        for value in inner_products:
            square = square - value * value
        length = jnp.sqrt(square)
        scale = jnp.where(opening, -1.0, 1.0) / length
        for known in range(KRYLOV):
            history[phase, known] = inner_products[known]
        history[phase, KRYLOV] = length

        @pl.when(phase < KRYLOV)
        def _():
            for side in range(2):
                whole = applied[side]
                for known in range(KRYLOV):
                    whole = whole - for_coefs(inner_products[known]) * vectors[known + 1, side]
                vectors[phase + 1, side] = for_coefs(scale) * whole
            receive_points()
            for pair in pairs:
                where = pair_rows(pair)
                fresh = []
                for part, whole in enumerate(points_of_rows(pair)):
                    for known in range(KRYLOV):
                        factor = for_points(inner_products[known])
                        whole = whole - factor * images[known + 1, part, where, :]
                    fresh.append(for_points(scale) * whole)
                    images[phase + 1, part, where, :] = fresh[part]
                crossed = images[0, 0, where, :] * fresh[1] + fresh[0] * images[0, 1, where, :]
                keep_product(pair, STRENGTH * crossed)
            send_products()

        @pl.when(phase == KRYLOV)
        def _():
            matrix = []
            for column in range(KRYLOV):
                entries = [history[column + 1, known] for known in range(column + 1)]
                matrix.append(entries + [history[column + 1, KRYLOV]])
            solved = least_squares(matrix, history[0, KRYLOV])
            @pl.when(index + 1 < steps)
            def _():
                for pair in pairs:
                    where = pair_rows(pair)
                    fresh = []
                    for part in range(2):
                        whole = images[0, part, where, :]
                        for known in range(KRYLOV):
                            factor = for_points(solved[known])
                            whole = whole + factor * images[known + 1, part, where, :]
                        fresh.append(whole)
                        images[0, part, where, :] = whole
                    keep_product(pair, STRENGTH * fresh[0] * fresh[1])
                send_products()

            for side in range(2):
                whole = vectors[0, side]
                for known in range(KRYLOV):
                    whole = whole + for_coefs(solved[known]) * vectors[known + 1, side]
                vectors[0, side] = whole

        return carry

    lax.fori_loop(0, steps, iteration, 0)
    for side in range(2):
        whole = vectors[0, side].reshape(LANES, degrees)
        ordered[side, 0] = whole[:, :LANES]
        ordered[side, 1] = whole[:, LANES:]
    for flow in range(2):
        for part in range(2):
            for side in range(2):
                where = pl.ds(2 * flow + part, half, stride=4)
                out_ref[flow, part, pl.ds(side * half, half), :] = jnp.concatenate(
                    [ordered[side, 0, where, :], ordered[side, 1, where, :]], axis=1
                )


def solve_flows(start, forcing, taus):
    group_size = lax.axis_size(AXES)
    minor = lax.axis_size(AXES[1])
    batch, parts, local_modes, degrees = start.shape
    rows = degrees // group_size
    inner = 2 * group_size
    half = local_modes // 2
    tables = tables_of(local_modes, group_size, degrees)
    sizes = (group_size, minor, local_modes, rows, degrees, inner)

    coefs = (2, LANES // 8, 8, degrees)

    field = (2, degrees, LANES)
    image = (2, rows * inner, LANES)
    chunk = 4 * degrees
    chunks = local_modes // 4
    vmem = pl.BlockSpec(memory_space=pltpu.VMEM)
    out = pl.pallas_call(
        functools.partial(flow_solver, sizes),
        out_shape=jax.ShapeDtypeStruct(start.shape, jnp.float32),
        in_specs=[vmem, vmem] + [pl.BlockSpec(memory_space=pl.ANY)] * (1 + len(tables)),
        out_specs=vmem,
        scratch_shapes=[pltpu.VMEM(table.shape, table.dtype) for table in tables]
        + [
            pltpu.VMEM((local_modes * 2 * degrees, degrees), jnp.bfloat16),
            pltpu.VMEM((chunks, chunk, degrees), jnp.float32),
            pltpu.VMEM((KRYLOV + 1,) + coefs, jnp.float32),
            pltpu.VMEM(coefs, jnp.float32),
            pltpu.VMEM((KRYLOV + 1, 8, LANES), jnp.float32),
            pltpu.VMEM(field, jnp.float32),
            pltpu.VMEM((KRYLOV + 1,) + image, jnp.float32),
            pltpu.VMEM((2, 2, LANES, LANES), jnp.float32),
            pltpu.VMEM((rows // 2, 4 * inner, 2 * LANES), jnp.float32),
            pltpu.VMEM((rows // 2, 4 * inner, 4 * LANES), jnp.bfloat16),
            pltpu.VMEM((rows // 2, 2 * inner, 3 * LANES), jnp.bfloat16),
            pltpu.VMEM((rows // 2, 6 * inner, 2 * LANES), jnp.bfloat16),
            pltpu.VMEM(field, jnp.float32),
            pltpu.VMEM(field, jnp.float32),
            pltpu.VMEM(field, jnp.float32),
            pltpu.VMEM(field, jnp.float32),
            pltpu.VMEM((1, LANES), jnp.float32),
            pltpu.VMEM((group_size, 1, LANES), jnp.float32),
            pltpu.VMEM((KRYLOV + 1, KRYLOV + 1, 16, LANES), jnp.float32),
            pltpu.SemaphoreType.DMA((chunks,)),
            pltpu.SemaphoreType.DMA((len(tables),)),
        ]
        + [pltpu.SemaphoreType.DMA((2,))] * 4
        + [pltpu.SemaphoreType.DMA] * 2,
        compiler_params=pltpu.CompilerParams(
            collective_id=0, has_side_effects=True, vmem_limit_bytes=56 * 1024 * 1024
        ),
    )(
        start,
        forcing,
        taus.reshape(local_modes * degrees, degrees),
        *[jnp.asarray(table) for table in tables],
    )
    return out


def fits_kernel(start):
    batch, parts, local_modes, degrees = start.shape
    group = lax.axis_size(AXES)
    rows = degrees // group
    fits = (batch, parts, rows, batch * local_modes) == (2, 2, 8, LANES)
    return fits and group & (group - 1) == 0


def local_step(start, forcing, taus):
    if fits_kernel(start):
        return solve_flows(start, forcing, taus)
    return shards(start, forcing, taus)


def solution(mesh):
    return jax.shard_map(
        local_step,
        mesh=mesh,
        in_specs=(
            P(None, None, ("modes", "cheb"), None),
            P(None, None, ("modes", "cheb"), None),
            P(("modes", "cheb"), None, None),
        ),
        out_specs=P(None, None, ("modes", "cheb"), None),
        check_vma=False,
    )
```

```python
import functools
import math

import jax
import jax.numpy as jnp
import numpy as np
from jax import lax
from jax.experimental import pallas as pl
from jax.experimental.pallas import tpu as pltpu
from jax.sharding import PartitionSpec as P

NEWTON = 2
KRYLOV = 3


PREC = lax.Precision.HIGH
STRENGTH = 0.1
AXES = ("modes", "cheb")
STAT_LANES = 128
LANES = 128


def cheb_rows(degree_count):
    degree = jnp.arange(degree_count, dtype=jnp.int32)[:, None]
    node = 2 * jnp.arange(degree_count, dtype=jnp.int32)[None, :] + 1
    turns = degree * node % (4 * degree_count)
    return jnp.cos(2.0 * math.pi / (4 * degree_count) * turns.astype(jnp.float32))


def phase_table(row_count, col_count, period):
    row_index = jnp.arange(row_count, dtype=jnp.int32)[:, None]
    col_index = jnp.arange(col_count, dtype=jnp.int32)[None, :]
    turns = row_index * col_index % period
    angle = 2.0 * math.pi / period * turns.astype(jnp.float32)
    return (jnp.cos(angle), jnp.sin(angle))


def least_squares(matrix, beta_norm):
    steps_count = len(matrix)
    target = [beta_norm] + [jnp.zeros_like(beta_norm) for row_index in range(steps_count)]
    cosines = []
    sines_list = []
    for col_index in range(steps_count):
        column = matrix[col_index]
        for row_index in range(col_index):
            upper_entry = (
                cosines[row_index] * column[row_index]
                + sines_list[row_index] * column[row_index + 1]
            )
            lower_entry = (
                cosines[row_index] * column[row_index + 1]
                - sines_list[row_index] * column[row_index]
            )
            column[row_index] = upper_entry
            column[row_index + 1] = lower_entry
        radius = jnp.sqrt(
            column[col_index] * column[col_index] + column[col_index + 1] * column[col_index + 1]
        )
        cosines.append(column[col_index] / radius)
        sines_list.append(column[col_index + 1] / radius)
        column[col_index] = radius
        target[col_index + 1] = -sines_list[col_index] * target[col_index]
        target[col_index] = cosines[col_index] * target[col_index]
    solved = [None] * steps_count
    for row_index in reversed(range(steps_count)):
        partial_sum = target[row_index]
        for col_index in range(row_index + 1, steps_count):
            partial_sum = partial_sum - matrix[col_index][row_index] * solved[col_index]
        solved[row_index] = partial_sum / matrix[row_index][row_index]
    return solved


def shards(start, forcing, taus):
    group_size = lax.axis_size(AXES)
    batch, parts, local_modes, degrees = start.shape
    total_modes = local_modes * group_size
    points_count = 2 * total_modes
    outer_len = max(2 ** ((points_count.bit_length() - 1) // 2), local_modes)
    inner_len = points_count // outer_len
    half_inner = inner_len // 2
    split = outer_len // local_modes
    rows = degrees // group_size
    block_lanes = batch * 2 * local_modes
    fields = rows * batch
    spread = 1.0 / math.sqrt(total_modes * degrees)
    gather_factor = math.sqrt(total_modes * degrees) / points_count
    cheb_table = cheb_rows(degrees)
    tau_keep = (jnp.arange(degrees) < degrees - 2).astype(jnp.float32)
    coef_weights = jnp.where(jnp.arange(degrees) == 0, 1.0, 2.0).astype(jnp.float32) / degrees
    back_table = cheb_table * (coef_weights * tau_keep)[:, None]

    section_cos, section_sin = phase_table(inner_len, half_inner, inner_len)
    value_table = jnp.stack([section_cos, section_sin])
    slope_table = jnp.stack([-section_sin, section_cos])
    back_cos, back_sin = section_cos.T, section_sin.T
    twist_cos, twist_sin = phase_table(inner_len, outer_len, points_count)
    final_cos, final_sin = phase_table(outer_len, outer_len, outer_len)
    turn_cos = (
        twist_cos[:, :, None] * final_cos[None] - twist_sin[:, :, None] * final_sin[None]
    )
    turn_sin = (
        twist_sin[:, :, None] * final_cos[None] + twist_cos[:, :, None] * final_sin[None]
    )
    turn_table = lax.optimization_barrier(
        jnp.concatenate([turn_cos, -turn_sin, -turn_sin, -turn_cos], axis=1)
    )
    mode = (
        outer_len * jnp.arange(half_inner, dtype=jnp.int32)[:, None]
        + jnp.arange(outer_len, dtype=jnp.int32)[None, :]
    )
    paired_mode = jnp.concatenate([mode, mode], axis=1)[:, None, :]
    weights = jnp.where(paired_mode == 0, 1.0, 2.0).astype(jnp.float32) * spread
    slope_weights = weights * (16.0 * paired_mode.astype(jnp.float32) / total_modes)

    def exchange(blocks):
        return lax.all_to_all(blocks, AXES, split_axis=0, concat_axis=0, tiled=True)

    def stat_block(stats):
        flat = jnp.pad(stats.reshape(-1), (0, STAT_LANES - stats.size))
        return jnp.broadcast_to(flat, (group_size, rows, STAT_LANES))

    def read_stats(received, shape):
        flat = jnp.sum(received[:, 0, :], axis=0)
        return flat[: math.prod(shape)].reshape(shape)

    def to_points(coefs, stats):
        values = jnp.einsum("ni,brkn->ibrk", cheb_table, coefs, precision=PREC)
        blocks = values.reshape(group_size, rows, block_lanes)
        if stats is not None:
            blocks = jnp.concatenate([blocks, stat_block(stats)], axis=2)
        received = exchange(blocks)
        summed = None
        if stats is not None:
            summed = read_stats(received[:, :, block_lanes:], stats.shape)
            received = received[:, :, :block_lanes]
        spectrum = received.reshape(half_inner, split, rows, batch, 2, local_modes)
        spectrum = spectrum.transpose(0, 2, 3, 4, 1, 5).reshape(
            half_inner, fields, 2 * outer_len
        )

        def points_of(table, weighted):
            turned = jnp.einsum("sjq,qyl->jysl", table, weighted, precision=PREC)
            turned = turned.reshape(inner_len, fields, 4 * outer_len)
            return jnp.einsum("jyl,jlt->jyt", turned, turn_table, precision=PREC)

        values = points_of(value_table, spectrum * weights)
        slopes = points_of(slope_table, spectrum * slope_weights)
        return (values, slopes), summed

    def to_coefficients(points):
        turned = jnp.einsum("jyt,jlt->jyl", points, turn_table, precision=PREC) * gather_factor
        direct = turned[:, :, : 2 * outer_len].reshape(inner_len, -1)
        swapped = turned[:, :, 2 * outer_len :].reshape(inner_len, -1)
        spectrum = jnp.dot(back_cos, direct, precision=PREC) + jnp.dot(
            back_sin, swapped, precision=PREC
        )
        blocks = spectrum.reshape(half_inner, rows, batch, 2, split, local_modes)
        blocks = blocks.transpose(0, 4, 1, 2, 3, 5).reshape(group_size, rows, block_lanes)
        received = exchange(blocks).reshape(degrees, batch, 2, local_modes)
        return jnp.einsum("ibrk,ni->brkn", received, back_table, precision=PREC)

    def precondition(coefs):
        return jnp.einsum("kam,brkm->brka", taus, coefs, precision=PREC)

    def on_points(scale):
        return jnp.tile(scale, rows)[None, :, None]

    def on_coefs(scale):
        return scale[:, None, None, None]

    iterate = start
    kept_forcing = forcing * tau_keep
    base, nothing = to_points(iterate, None)
    for newton_step in range(NEWTON):
        base_points, base_slopes = base
        residual = iterate + precondition(
            to_coefficients(STRENGTH * base_points * base_slopes) - kept_forcing
        )
        local_square = jnp.sum(residual * residual, axis=(1, 2, 3))
        image, squared = to_points(residual, local_square)
        beta_norm = jnp.sqrt(squared)
        krylov_basis = [-residual / on_coefs(beta_norm)]
        images = [tuple(-part / on_points(beta_norm) for part in image)]
        hessen = []
        for column in range(KRYLOV):
            probe_points, probe_slopes = images[column]
            product = STRENGTH * (base_points * probe_slopes + probe_points * base_slopes)
            applied = krylov_basis[column] + precondition(to_coefficients(product))
            local_stats = jnp.stack(
                [jnp.sum(vector * applied, axis=(1, 2, 3)) for vector in krylov_basis + [applied]],
                axis=1,
            )
            last = column == KRYLOV - 1
            if last:
                stats = read_stats(exchange(stat_block(local_stats)), local_stats.shape)
            else:
                image, stats = to_points(applied, local_stats)
            projections, square = stats[:, :-1], stats[:, -1]
            length = jnp.sqrt(square - jnp.sum(projections * projections, axis=1))
            hessen.append(jnp.concatenate([projections, length[:, None]], axis=1))
            if not last:
                for index in range(column + 1):
                    applied = applied - on_coefs(projections[:, index]) * krylov_basis[index]
                    image = tuple(
                        part - on_points(projections[:, index]) * known
                        for part, known in zip(image, images[index])
                    )
                krylov_basis.append(applied / on_coefs(length))
                images.append(tuple(part / on_points(length) for part in image))
        matrix = [
            [hessen[column][:, row] for row in range(column + 2)] for column in range(KRYLOV)
        ]
        solved = least_squares(matrix, beta_norm)
        for column in range(KRYLOV):
            iterate = iterate + on_coefs(solved[column]) * krylov_basis[column]
            base = tuple(
                part + on_points(solved[column]) * known
                for part, known in zip(base, images[column])
            )
    return iterate


def split_table(table):
    table = np.asarray(table, np.float32)
    high = table.astype(jnp.bfloat16)
    low = (table - high.astype(np.float32)).astype(jnp.bfloat16)
    return high, low


def left_table(table):
    high, low = split_table(table)
    return np.concatenate([high, low, high], axis=1)


def tables_of(local_modes, group_size, degrees):
    total = local_modes * group_size
    points = 2 * total
    inner = points // local_modes
    half = local_modes // 2
    spread = 1.0 / math.sqrt(total * degrees)
    degree = np.arange(degrees)[:, None]
    node = 2 * np.arange(degrees)[None, :] + 1
    cheb = np.cos(2.0 * np.pi / (4 * degrees) * (degree * node % (4 * degrees)))
    coef_weights = np.where(np.arange(degrees) == 0, 1.0, 2.0) / degrees
    keep = np.arange(degrees) < degrees - 2
    to_rows = left_table(cheb.T)
    to_degrees = left_table((cheb * (coef_weights * keep)[:, None]).T)

    j_low = np.arange(inner)[:, None]
    source = np.arange(group_size)[None, :]
    angle = 2.0 * np.pi / inner * (j_low * source % inner)
    cos, sin = np.cos(angle), np.sin(angle)
    real = np.concatenate([cos, -sin], axis=1)
    imag = np.concatenate([sin, cos], axis=1)
    wave = np.tile(16.0 * local_modes * source / total, (1, 2))
    gather = 2.0 * spread * np.concatenate([real, imag, real * wave, imag * wave], axis=0)
    gather = left_table(gather)
    scatter = np.concatenate(
        [np.concatenate([cos.T, sin.T], axis=1), np.concatenate([-sin.T, cos.T], axis=1)], axis=0
    )
    scatter = left_table(scatter * math.sqrt(total * degrees) / points)

    lane = np.arange(2 * local_modes)
    lane_mode = (lane // 4 + half * (lane % 2))[None, :]
    lane_flow = lane // 2 % 2
    twist = 2.0 * np.pi / points * (j_low * lane_mode)
    wave_low = np.broadcast_to(16.0 * lane_mode / total, twist.shape)
    twist = np.stack([np.cos(twist), np.sin(twist), wave_low]).astype(np.float32)

    final = lane_mode.T * np.tile(np.arange(local_modes), 2)[None, :] % local_modes
    final = 2.0 * np.pi / local_modes * final
    same = lane_flow[:, None] == lane[None, :] // local_modes
    cos_high, cos_low = split_table(same * np.cos(final))
    sin_high, sin_low = split_table(same * np.sin(final))
    cos_row = np.concatenate([cos_high, cos_low], axis=1)
    sin_row = np.concatenate([-sin_high, -sin_low], axis=1)
    finish = np.concatenate([cos_row, sin_row, cos_row, sin_row], axis=0)
    high_row = np.concatenate([cos_high.T, -sin_high.T], axis=1)
    low_row = np.concatenate([cos_low.T, -sin_low.T], axis=1)
    begin = np.concatenate([high_row, high_row, low_row], axis=0)
    return to_rows, to_degrees, gather, scatter, twist, finish, begin


def split(value):
    high = value.astype(jnp.bfloat16)
    return high, (value - high.astype(jnp.float32)).astype(jnp.bfloat16)


def right_operand(value):
    high, low = split(value)
    return jnp.concatenate([high, high, low], axis=0)


def dot(left, right):
    return jnp.dot(left, right, preferred_element_type=jnp.float32)


def dot_rows(left, right):
    dims = (((1,), (1,)), ((), ()))
    return lax.dot_general(left, right, dims, preferred_element_type=jnp.float32)


def row_operand(value):
    high, low = split(value)
    return jnp.concatenate([high, high, low], axis=1)


def flow_solver(
    sizes,
    start_ref,
    forcing_ref,
    taus_ref,
    to_rows_hbm,
    to_degrees_hbm,
    gather_hbm,
    scatter_hbm,
    twist_hbm,
    finish_hbm,
    begin_hbm,
    out_ref,
    to_rows_ref,
    to_degrees_ref,
    gather_ref,
    scatter_ref,
    twist_ref,
    finish_ref,
    begin_ref,
    tau_terms,
    stage,
    vectors,
    applied,
    partial,
    driven,
    images,
    ordered,
    summed,
    lefts,
    products,
    rights,
    out_fwd,
    in_fwd,
    out_back,
    in_back,
    out_stat,
    in_stat,
    history,
    stage_sem,
    table_sem,
    fwd_send,
    fwd_recv,
    back_send,
    back_recv,
    stat_send,
    stat_recv,
):
    group_size, minor, local_modes, rows, degrees, inner = sizes
    half = local_modes // 2
    me = lax.axis_index(AXES[0]) * minor + lax.axis_index(AXES[1])
    lane = lax.broadcasted_iota(jnp.int32, (1, LANES), 1)
    even_lane = lane % 2 == 0
    low_flow = lane < local_modes
    low_rows = lax.broadcasted_iota(jnp.int32, (8, LANES), 0) % 4 < 2

    def own_rows(index):
        return pl.ds(pl.multiple_of(index * rows, rows), rows)

    flips = []
    for bit in range(group_size.bit_length() - 1):
        flips.append((1 << bit) - (2 << bit) * lax.rem(me // (1 << bit), 2))

    def peers():
        for distance in reversed(range(1, group_size)):
            peer = me
            for bit, flip in enumerate(flips):
                if distance >> bit & 1:
                    peer = peer + flip
            yield peer, (peer // minor, lax.rem(peer, minor))

    def exchange(src, dst, send_sem, recv_sem):
        for peer, place in peers():
            pltpu.make_async_remote_copy(
                src_ref=src.at[own_rows(peer), :],
                dst_ref=dst.at[own_rows(me), :],
                send_sem=send_sem,
                recv_sem=recv_sem,
                device_id=place,
                device_id_type=pl.DeviceIdType.MESH,
            ).start()
        pltpu.make_async_copy(
            src.at[own_rows(me), :], dst.at[own_rows(me), :], recv_sem
        ).start()

    def finish_exchange(src, dst, send_sem, recv_sem):
        sent = pl.ds(0, (group_size - 1) * rows)
        pltpu.make_async_copy(src.at[sent, :], dst.at[sent, :], send_sem).wait()
        pltpu.make_async_copy(src, dst, recv_sem).wait()

    def to_modes(first, second):
        turned = pltpu.roll(second, 1, 1)
        back = pltpu.roll(first, LANES - 1, 1)
        return jnp.where(even_lane, first, turned), jnp.where(even_lane, back, second)

    def rows_of(field):
        return dot_rows(to_rows_ref[...], row_operand(field.reshape(LANES, degrees)))

    def send_values(side, field):
        constant = jnp.logical_and(me + side == 0, lane < 4)
        out_fwd[side] = rows_of(field) * jnp.where(constant, 0.5, 1.0)
        exchange(out_fwd.at[side], in_fwd.at[side], fwd_send.at[side], fwd_recv.at[side])

    pairs = range(rows // 2)

    def sums_over_sources():
        for pair in pairs:
            columns = []
            for row in (2 * pair, 2 * pair + 1):
                picked = pl.ds(row, group_size, stride=rows)
                real, imag = to_modes(in_fwd[0, picked, :], in_fwd[1, picked, :])
                columns.append(jnp.concatenate([real, imag], axis=0))
            operand = right_operand(jnp.concatenate(columns, axis=1))
            summed[pair] = dot(gather_ref[...], operand)
        cos, sin, low = twist_ref[0], twist_ref[1], twist_ref[2]
        for row in range(rows):
            pair, index = divmod(row, 2)
            lanes = slice(index * LANES, (index + 1) * LANES)
            real, imag, wave_real, wave_imag = (
                summed[pair, n * inner : (n + 1) * inner, lanes] for n in range(4)
            )
            slope_real = -(wave_imag + low * imag)
            slope_imag = wave_real + low * real
            for part, (re, im) in enumerate(((real, imag), (slope_real, slope_imag))):
                re_high, re_low = split(re * cos - im * sin)
                im_high, im_low = split(re * sin + im * cos)
                where = slice((2 * part + index) * inner, (2 * part + index + 1) * inner)
                lefts[pair, where] = jnp.concatenate([re_high, im_high, re_low, im_low], axis=1)

    def points_of_rows(pair):
        wide = dot(lefts[pair], finish_ref[...])
        points = wide[:, :LANES] + wide[:, LANES:]
        return points[: 2 * inner], points[2 * inner :]

    def receive_points():
        for side in range(2):
            finish_exchange(
                out_fwd.at[side], in_fwd.at[side], fwd_send.at[side], fwd_recv.at[side]
            )
        sums_over_sources()

    def pair_rows(pair):
        return pl.ds(2 * pair * inner, 2 * inner)

    def keep_product(pair, product):
        high, low = split(product)
        products[pair] = jnp.concatenate([high, low, high], axis=1)

    def send_products():
        cos, sin = twist_ref[0], twist_ref[1]
        for pair in pairs:
            turned = dot(products[pair], begin_ref[...])
            columns = []
            for index in range(2):
                part = turned[index * inner : (index + 1) * inner]
                real, imag = part[:, :LANES], part[:, LANES:]
                columns.append(
                    jnp.concatenate([real * cos + imag * sin, imag * cos - real * sin], axis=0)
                )
            rights[pair] = right_operand(jnp.concatenate(columns, axis=1))
        for pair in pairs:
            spread = dot(scatter_ref[...], rights[pair])
            for index in range(2):
                part = spread[:, index * LANES : (index + 1) * LANES]
                first, second = to_modes(part[:group_size], part[group_size:])
                picked = pl.ds(2 * pair + index, group_size, stride=rows)
                out_back[0, picked, :] = first
                out_back[1, picked, :] = second
        for side in range(2):
            exchange(out_back.at[side], in_back.at[side], back_send.at[side], back_recv.at[side])

    top_rows = lax.broadcasted_iota(jnp.int32, (8, degrees), 0) < 4

    def precondition(side, field):
        high = field.astype(jnp.bfloat16).astype(jnp.float32)
        terms = [part.reshape(LANES // 8, 8, degrees) for part in (high, field - high)]
        terms = jnp.stack(terms, axis=1).reshape(2 * LANES, degrees).astype(jnp.bfloat16)
        for pair in range(half // 2):
            left = terms[16 * pair : 16 * pair + 16]
            left = jnp.concatenate([left, left], axis=1)
            found = []
            for index in range(2):
                base = (side * half + 2 * pair + index) * 2 * degrees
                where = pl.ds(pl.multiple_of(base, 2 * degrees), 2 * degrees)
                both = dot(left, tau_terms[where, :])
                found.append(both[:8] + both[8:])
            applied[side, pair] = jnp.where(top_rows, found[0], found[1])

    stat_row = lax.broadcasted_iota(jnp.int32, (8, LANES), 0)
    packed = stat_row == lax.broadcasted_iota(jnp.int32, (8, LANES), 1)

    def send_stats():
        sums = []
        for chosen in (low_rows, ~low_rows):
            for known in range(KRYLOV + 1):
                sums.append(
                    jnp.sum(jnp.where(chosen, partial[known], 0.0), axis=0, keepdims=True)
                )
        sums = jnp.sum(jnp.concatenate(sums, axis=0), axis=1, keepdims=True)
        out_stat[...] = jnp.sum(jnp.where(packed, sums, 0.0), axis=0, keepdims=True)
        for peer, place in peers():
            pltpu.make_async_remote_copy(
                src_ref=out_stat,
                dst_ref=in_stat.at[me],
                send_sem=stat_send,
                recv_sem=stat_recv,
                device_id=place,
                device_id_type=pl.DeviceIdType.MESH,
            ).start()
        pltpu.make_async_copy(out_stat, in_stat.at[me], stat_recv).start()

    def receive_stats():
        sent = pl.ds(0, group_size - 1)
        pltpu.make_async_copy(in_stat.at[sent], in_stat.at[sent], stat_send).wait()
        pltpu.make_async_copy(in_stat, in_stat, stat_recv).wait()
        total = jnp.sum(in_stat[...], axis=0)
        return jnp.sum(jnp.where(packed, total, 0.0), axis=1, keepdims=True)

    def by_flow(stats, known):
        low = jnp.broadcast_to(stats[known : known + 1], (8, LANES))
        high = jnp.broadcast_to(stats[known + KRYLOV + 1 : known + KRYLOV + 2], (8, LANES))
        return jnp.concatenate(
            [jnp.where(low_flow, low, high), jnp.where(low_rows, low, high)], axis=0
        )

    def for_points(value):
        return value[:1]

    def for_coefs(value):
        return jnp.concatenate([value[8:], value[8:]], axis=1)[None]

    chunks, chunk = stage.shape[:2]

    def fetch(index):
        where = pl.ds(pl.multiple_of(index * chunk, chunk), chunk)
        return pltpu.make_async_copy(taus_ref.at[where, :], stage.at[index], stage_sem.at[index])

    def fetch_step(index, carry):
        fetch(index).start()
        return carry

    barrier = pltpu.get_barrier_semaphore()
    for _, place in peers():
        pl.semaphore_signal(
            barrier, inc=1, device_id=place, device_id_type=pl.DeviceIdType.MESH
        )
    tables = (
        (to_rows_hbm, to_rows_ref),
        (to_degrees_hbm, to_degrees_ref),
        (gather_hbm, gather_ref),
        (scatter_hbm, scatter_ref),
        (twist_hbm, twist_ref),
        (finish_hbm, finish_ref),
        (begin_hbm, begin_ref),
    )
    tables = [
        pltpu.make_async_copy(src, dst, table_sem.at[index])
        for index, (src, dst) in enumerate(tables)
    ]
    for copy in tables:
        copy.start()
    lax.fori_loop(0, chunks, fetch_step, 0)

    def spread_rows(field_ref):
        for flow in range(2):
            for part in range(2):
                for side in range(2):
                    rows_of_part = field_ref[flow, part, pl.ds(side * half, half), :]
                    where = pl.ds(2 * flow + part, half, stride=4)
                    for column in range(2):
                        lanes = slice(column * LANES, (column + 1) * LANES)
                        ordered[side, column, where, :] = rows_of_part[:, lanes]

    def in_order(side):
        return jnp.concatenate([ordered[side, 0], ordered[side, 1]], axis=1)

    vectors[...] = jnp.zeros_like(vectors)
    images[...] = jnp.zeros_like(images)
    spread_rows(start_ref)
    for copy in tables:
        copy.wait()
    pl.semaphore_wait(barrier, group_size - 1)
    for side in range(2):
        vectors[0, side] = in_order(side).reshape(LANES // 8, 8, degrees)
    for side in range(2):
        send_values(side, vectors[0, side])
    spread_rows(forcing_ref)
    for side in range(2):
        driven[side] = rows_of(in_order(side))

    def load(index, carry):
        fetch(index).wait()
        for mode in range(chunk // degrees):
            operand = row_operand(stage[index, mode * degrees : (mode + 1) * degrees])
            high, low = split(dot_rows(to_degrees_ref[...], operand))
            base = (index * (chunk // degrees) + mode) * 2 * degrees
            base = pl.multiple_of(base, 2 * degrees)
            tau_terms[pl.ds(base, degrees), :] = high
            tau_terms[pl.ds(base + degrees, degrees), :] = low
        return carry

    lax.fori_loop(0, chunks // 2, load, 0)

    receive_points()
    for pair in pairs:
        points = points_of_rows(pair)
        for part in range(2):
            images[0, part, pair_rows(pair), :] = points[part]
        keep_product(pair, STRENGTH * points[0] * points[1])
    send_products()
    steps = NEWTON * (KRYLOV + 1)

    def iteration(index, carry):
        phase = lax.rem(index, KRYLOV + 1)
        opening = phase == 0

        @pl.when(index == 0)
        def _():
            lax.fori_loop(chunks // 2, chunks, load, 0)

        drive = jnp.where(opening, 1.0, 0.0)
        partial[...] = jnp.zeros_like(partial)

        def half_step(side, carry):
            finish_exchange(
                out_back.at[side], in_back.at[side], back_send.at[side], back_recv.at[side]
            )
            precondition(side, (in_back[side] - drive * driven[side]).T)
            whole = vectors[phase, side] + applied[side]
            applied[side] = whole

            @pl.when(phase < KRYLOV)
            def _():
                send_values(side, applied[side])

            def add_stat(known, other):
                summed = jnp.sum(other * whole, axis=0)
                partial[known] += summed[:, :LANES] + summed[:, LANES:]

            for known in range(KRYLOV):
                add_stat(known, vectors[known + 1, side])
            add_stat(KRYLOV, whole)

            @pl.when(side == 1)
            def _():
                send_stats()

            return carry

        lax.fori_loop(0, 2, half_step, 0)
        @pl.when(phase < KRYLOV)
        def _():
            receive_points()

        stats = receive_stats()
        inner_products = [
            jnp.where(known < phase, by_flow(stats, known), 0.0) for known in range(KRYLOV)
        ]
        square = by_flow(stats, KRYLOV)
        for value in inner_products:
            square = square - value * value
        length = jnp.sqrt(square)
        scale = jnp.where(opening, -1.0, 1.0) / length
        for known in range(KRYLOV):
            history[phase, known] = inner_products[known]
        history[phase, KRYLOV] = length

        @pl.when(phase < KRYLOV)
        def _():
            for pair in pairs:
                where = pair_rows(pair)
                fresh = []
                for part, whole in enumerate(points_of_rows(pair)):
                    for known in range(KRYLOV):
                        factor = for_points(inner_products[known])
                        whole = whole - factor * images[known + 1, part, where, :]
                    fresh.append(for_points(scale) * whole)
                    images[phase + 1, part, where, :] = fresh[part]
                crossed = images[0, 0, where, :] * fresh[1] + fresh[0] * images[0, 1, where, :]
                keep_product(pair, STRENGTH * crossed)
            send_products()
            for side in range(2):
                whole = applied[side]
                for known in range(KRYLOV):
                    whole = whole - for_coefs(inner_products[known]) * vectors[known + 1, side]
                vectors[phase + 1, side] = for_coefs(scale) * whole

        @pl.when(phase == KRYLOV)
        def _():
            matrix = []
            for column in range(KRYLOV):
                entries = [history[column + 1, known] for known in range(column + 1)]
                matrix.append(entries + [history[column + 1, KRYLOV]])
            solved = least_squares(matrix, history[0, KRYLOV])
            @pl.when(index + 1 < steps)
            def _():
                for pair in pairs:
                    where = pair_rows(pair)
                    fresh = []
                    for part in range(2):
                        whole = images[0, part, where, :]
                        for known in range(KRYLOV):
                            factor = for_points(solved[known])
                            whole = whole + factor * images[known + 1, part, where, :]
                        fresh.append(whole)
                        images[0, part, where, :] = whole
                    keep_product(pair, STRENGTH * fresh[0] * fresh[1])
                send_products()

            for side in range(2):
                whole = vectors[0, side]
                for known in range(KRYLOV):
                    whole = whole + for_coefs(solved[known]) * vectors[known + 1, side]
                vectors[0, side] = whole

        return carry

    lax.fori_loop(0, steps, iteration, 0)
    for side in range(2):
        whole = vectors[0, side].reshape(LANES, degrees)
        ordered[side, 0] = whole[:, :LANES]
        ordered[side, 1] = whole[:, LANES:]
    for flow in range(2):
        for part in range(2):
            for side in range(2):
                where = pl.ds(2 * flow + part, half, stride=4)
                out_ref[flow, part, pl.ds(side * half, half), :] = jnp.concatenate(
                    [ordered[side, 0, where, :], ordered[side, 1, where, :]], axis=1
                )


def solve_flows(start, forcing, taus):
    group_size = lax.axis_size(AXES)
    minor = lax.axis_size(AXES[1])
    batch, parts, local_modes, degrees = start.shape
    rows = degrees // group_size
    inner = 2 * group_size
    half = local_modes // 2
    tables = tables_of(local_modes, group_size, degrees)
    sizes = (group_size, minor, local_modes, rows, degrees, inner)

    coefs = (2, LANES // 8, 8, degrees)

    field = (2, degrees, LANES)
    image = (2, rows * inner, LANES)
    chunk = 4 * degrees
    chunks = local_modes // 4
    vmem = pl.BlockSpec(memory_space=pltpu.VMEM)
    out = pl.pallas_call(
        functools.partial(flow_solver, sizes),
        out_shape=jax.ShapeDtypeStruct(start.shape, jnp.float32),
        in_specs=[vmem, vmem] + [pl.BlockSpec(memory_space=pl.ANY)] * (1 + len(tables)),
        out_specs=vmem,
        scratch_shapes=[pltpu.VMEM(table.shape, table.dtype) for table in tables]
        + [
            pltpu.VMEM((local_modes * 2 * degrees, degrees), jnp.bfloat16),
            pltpu.VMEM((chunks, chunk, degrees), jnp.float32),
            pltpu.VMEM((KRYLOV + 1,) + coefs, jnp.float32),
            pltpu.VMEM(coefs, jnp.float32),
            pltpu.VMEM((KRYLOV + 1, 8, LANES), jnp.float32),
            pltpu.VMEM(field, jnp.float32),
            pltpu.VMEM((KRYLOV + 1,) + image, jnp.float32),
            pltpu.VMEM((2, 2, LANES, LANES), jnp.float32),
            pltpu.VMEM((rows // 2, 4 * inner, 2 * LANES), jnp.float32),
            pltpu.VMEM((rows // 2, 4 * inner, 4 * LANES), jnp.bfloat16),
            pltpu.VMEM((rows // 2, 2 * inner, 3 * LANES), jnp.bfloat16),
            pltpu.VMEM((rows // 2, 6 * inner, 2 * LANES), jnp.bfloat16),
            pltpu.VMEM(field, jnp.float32),
            pltpu.VMEM(field, jnp.float32),
            pltpu.VMEM(field, jnp.float32),
            pltpu.VMEM(field, jnp.float32),
            pltpu.VMEM((1, LANES), jnp.float32),
            pltpu.VMEM((group_size, 1, LANES), jnp.float32),
            pltpu.VMEM((KRYLOV + 1, KRYLOV + 1, 16, LANES), jnp.float32),
            pltpu.SemaphoreType.DMA((chunks,)),
            pltpu.SemaphoreType.DMA((len(tables),)),
        ]
        + [pltpu.SemaphoreType.DMA((2,))] * 4
        + [pltpu.SemaphoreType.DMA] * 2,
        compiler_params=pltpu.CompilerParams(
            collective_id=0, has_side_effects=True, vmem_limit_bytes=56 * 1024 * 1024
        ),
    )(
        start,
        forcing,
        taus.reshape(local_modes * degrees, degrees),
        *[jnp.asarray(table) for table in tables],
    )
    return out


def fits_kernel(start):
    batch, parts, local_modes, degrees = start.shape
    group = lax.axis_size(AXES)
    rows = degrees // group
    fits = (batch, parts, rows, batch * local_modes) == (2, 2, 8, LANES)
    return fits and group & (group - 1) == 0


def local_step(start, forcing, taus):
    if fits_kernel(start):
        return solve_flows(start, forcing, taus)
    return shards(start, forcing, taus)


def solution(mesh):
    return jax.shard_map(
        local_step,
        mesh=mesh,
        in_specs=(
            P(None, None, ("modes", "cheb"), None),
            P(None, None, ("modes", "cheb"), None),
            P(("modes", "cheb"), None, None),
        ),
        out_specs=P(None, None, ("modes", "cheb"), None),
        check_vma=False,
    )
```
